32 devices in a mesh: narrow: 4 (over z), wide: 8 (over y, x, core).
Axes of the slice: x: 2, y: 2, z: 4, core: 2. Of those that a mesh axis runs over, the one named last changes fastest.
Arguments:
- hidden_in: bfloat16 [8, 2048, 2048], P('narrow', 'wide'), may hold values from -6 to 6
- out_grad: bfloat16 [8, 2048, 2048], P('narrow', 'wide'), may hold values from -6 to 6
- doc_lengths: int32 [8, 8], P('narrow'), may hold values from 1 to 1024, 2048 in all within a row
- attn_gain: bfloat16 [2048], P('narrow'), may hold values from 0.5 to 1.5
- w_query: bfloat16 [2048, 2048], P('narrow', 'wide'), may hold values from -0.125 to 0.125
- w_key: bfloat16 [2048, 2048], P('narrow', 'wide'), may hold values from -0.125 to 0.125
- w_value: bfloat16 [2048, 2048], P('narrow', 'wide'), may hold values from -0.125 to 0.125
- w_out: bfloat16 [2048, 2048], P('wide', 'narrow'), may hold values from -1 to 1
- mlp_gain: bfloat16 [2048], P('narrow'), may hold values from 0.5 to 1.5
- w_gate: bfloat16 [2048, 8192], P('narrow', 'wide'), may hold values from -0.125 to 0.125
- w_up: bfloat16 [2048, 8192], P('narrow', 'wide'), may hold values from -0.125 to 0.125
- w_down: bfloat16 [8192, 2048], P('wide', 'narrow'), may hold values from -0.0625 to 0.0625
Outputs:
- hidden_out: bfloat16 [8, 2048, 2048], P('narrow', 'wide')
- in_grad: bfloat16 [8, 2048, 2048], P('narrow', 'wide')
- grad_attn_gain: float32 [2048], P(('narrow', 'wide'))
- grad_w_query: float32 [2048, 2048], P('narrow', 'wide')
- grad_w_key: float32 [2048, 2048], P('narrow', 'wide')
- grad_w_value: float32 [2048, 2048], P('narrow', 'wide')
- grad_w_out: float32 [2048, 2048], P('wide', 'narrow')
- grad_mlp_gain: float32 [2048], P(('narrow', 'wide'))
- grad_w_gate: float32 [2048, 8192], P('narrow', 'wide')
- grad_w_up: float32 [2048, 8192], P('narrow', 'wide')
- grad_w_down: float32 [8192, 2048], P('wide', 'narrow')
The draws below stay inside these ranges and needn't reach their ends.
Inputs may be any that keep to these rules, and one draw needn't show every extreme that they name: `doc_lengths`: in every row the 8 lengths sum to 2048, and the longest is exactly 1024.
All inputs are finite; a program needn't handle non-finite values.
Results may differ from the reference program's by a relative error of at most 0.029.
Values may be sent and summed in bfloat16 or wider, within the bound.
No kernel may reach another device: no remote copies, remote signals or barrier semaphores. Data moves between devices by JAX's collectives and lax.ppermute only.
A program may use at most 192 MiB of HBM per device.

```python
import math
import jax
import jax.numpy as jnp
import numpy as np
from jax import lax

D = 2048
HEADS = 32
HEAD_DIM = 64
FF = 8192
SEQ = 2048
DOCS = 8
ROWS = 8
GROUPS = 8


def block_scale(rng, shape, pieces, least, top_value):
    factor_of = 1.0
    for axis_at, blocks in pieces:
        heights = jax.random.uniform(jax.random.fold_in(jax.random.fold_in(rng, 6), axis_at), (blocks,), jnp.float32, least / len(pieces), top_value / len(pieces))
        factor_of = factor_of * jnp.repeat(jnp.exp(heights), shape[axis_at] // blocks).reshape((-1,) + (1,) * (len(shape) - 1 - axis_at))
    return factor_of


def length_profile(amount, total, reach, skew):
    loads = [(1 << 20) // math.isqrt(standing ** skew) + 1 for standing in range(2, amount + 1)]
    surplus, given = total - reach - (amount - 1), [1] * (amount - 1)
    while surplus > 0:
        candidates = [i for i in range(amount - 1) if given[i] < reach]
        mass, budget = sum([loads[i] for i in candidates]), surplus
        for i in candidates:
            addition = min(reach - given[i], max(1, budget * loads[i] // mass), surplus)
            given[i] = given[i] + addition
            surplus = surplus - addition
    return np.array([reach] + given)


def uneven(stream_key, count, total, limit, slope):
    if count == 2:
        one = jax.random.randint(stream_key, (), max(1, total - limit), min(limit, total - 1) + 1)
        return jnp.stack([one, total - one])
    sizes = jnp.asarray(length_profile(count, total, limit, slope), jnp.int32)
    pairs = (count - 1) // 2
    source_of, taker = sizes[1:1 + 2 * pairs:2], sizes[2:2 + 2 * pairs:2]
    slack = jnp.minimum(source_of - 1, limit - taker)
    moved = jax.random.randint(jax.random.fold_in(stream_key, 1), (pairs,), 0, 1 << 20) % (slack + 1)
    sizes = sizes.at[1:1 + 2 * pairs:2].set(source_of - moved).at[2:2 + 2 * pairs:2].set(taker + moved)
    return sizes[jax.random.permutation(jax.random.fold_in(stream_key, 2), count)]


def normal_values(stream_key, shape, scale, bound, cuts=(), kind=jnp.bfloat16):
    values = jax.random.normal(stream_key, shape, jnp.float32) * scale
    if len(cuts) > 0:
        values = block_scale(stream_key, shape, cuts, -0.22, 0.18) * values
    return jnp.clip(values, min=-bound, max=bound).astype(kind)


def setup_inputs(seed: int = 0) -> dict:
    key_of = jax.random.split(jax.random.key(seed), 13)
    return {
        "hidden_in": normal_values(key_of[0], (ROWS, SEQ, D), 1.0, 6.0, ((0, 4), (1, 8))),
        "out_grad": normal_values(key_of[1], (ROWS, SEQ, D), 1.0, 6.0, ((0, 4), (1, 8))),
        "doc_lengths": jax.vmap(lambda own: uneven(own, DOCS, SEQ, SEQ // 2, 2))(jax.random.split(key_of[2], ROWS)).reshape((ROWS, DOCS)).astype(jnp.int32),
        "attn_gain": jnp.clip(1.0 + 0.1 * jax.random.normal(key_of[3], (D,), jnp.float32), 0.5, 1.5).astype(jnp.bfloat16),
        "w_query": normal_values(key_of[4], (D, D), D ** -0.5, 0.125, ((0, 4), (1, 8))),
        "w_key": normal_values(key_of[5], (D, D), D ** -0.5, 0.125, ((0, 4), (1, 8))),
        "w_value": normal_values(key_of[6], (D, D), D ** -0.5, 0.125, ((0, 4), (1, 8))),
        "w_out": normal_values(key_of[7], (D, D), (D // 64) ** -0.5, 1.0, ((0, 8), (1, 4))),
        "mlp_gain": jnp.clip(1.0 + 0.1 * jax.random.normal(key_of[8], (D,), jnp.float32), 0.5, 1.5).astype(jnp.bfloat16),
        "w_gate": normal_values(key_of[9], (D, FF), D ** -0.5, 0.125, ((0, 4), (1, 8))),
        "w_up": normal_values(key_of[10], (D, FF), D ** -0.5, 0.125, ((0, 4), (1, 8))),
        "w_down": normal_values(key_of[11], (FF, D), FF ** -0.5, 0.0625, ((0, 8), (1, 4))),
    }


EPS = 1e-05
NEG = -1e+30
ROPE_BASE = 130000.0
PRECISE = lax.Precision.HIGHEST

@jax.custom_vjp
def low(v):
    return lax.optimization_barrier(v.astype(jnp.bfloat16)).astype(jnp.float32)

@jax.custom_vjp
def low_back(v):
    return v

def low_keep(v):
    return (low(v), None)

def low_pass(kept, grad):
    return (grad,)

def back_keep(v):
    return (v, None)

def back_low(kept, grad):
    return (low(grad),)
low.defvjp(low_keep, low_pass)
low_back.defvjp(back_keep, back_low)

def mat_high(left_op, right_op):
    return jnp.dot(left_op, right_op, precision=PRECISE)

def doc_starts(lengths):
    tokens = jnp.arange(SEQ, dtype=jnp.int32)
    ends_at = jnp.cumsum(lengths).astype(jnp.int32)
    before = jnp.where(ends_at[None, :] <= tokens[:, None], ends_at[None, :], jnp.int32(0))
    return lax.optimization_barrier(jnp.max(before, axis=1)).astype(jnp.int32)

def rope_tables(starts):
    half_dim = HEAD_DIM // 2
    position = (jnp.arange(SEQ, dtype=jnp.int32) - starts).astype(jnp.float32)
    inverse = ROPE_BASE ** (-(jnp.arange(half_dim, dtype=jnp.float32) * 2.0) / HEAD_DIM)
    angles = position[:, None] * inverse[None, :]
    return (jnp.cos(angles)[:, None, :], jnp.sin(angles)[:, None, :])

def rotate(tensor, cos_table, sin_table):
    half_dim = tensor.shape[-1] // 2
    front_half = tensor[..., :half_dim]
    back_half = tensor[..., half_dim:]
    return jnp.concatenate([front_half * cos_table - back_half * sin_table, back_half * cos_table + front_half * sin_table], axis=-1)

def attention(queries, keys_rot, values_in, starts):
    block_len = min(512, SEQ)
    n_blocks = SEQ // block_len
    score_scale = HEAD_DIM ** (-0.5)
    blocks = queries.reshape(n_blocks, block_len, HEADS, HEAD_DIM)
    firsts = jnp.arange(n_blocks, dtype=jnp.int32) * block_len
    columns = jnp.arange(SEQ, dtype=jnp.int32)

    def one_block(block_pair):
        q_block, first_row = block_pair
        row_ids = first_row + jnp.arange(block_len, dtype=jnp.int32)
        begins = lax.dynamic_slice_in_dim(starts, first_row, block_len)
        allowed = (columns[None, :] <= row_ids[:, None]) & (columns[None, :] >= begins[:, None])
        scores = low_back(score_scale * jnp.einsum('qhd,khd->hqk', q_block, keys_rot, precision=PRECISE))
        masked = jnp.where(allowed[None], scores, NEG)
        row_max = lax.optimization_barrier(jnp.max(masked, axis=-1, keepdims=True))
        exp_terms = jnp.exp(masked - row_max)
        prob_rows = low(exp_terms / lax.optimization_barrier(jnp.sum(exp_terms, axis=-1, keepdims=True)))
        return jnp.einsum('hqk,khd->qhd', prob_rows, values_in, precision=PRECISE)
    block_outs = lax.map(jax.checkpoint(one_block), (blocks, firsts))
    return block_outs.reshape(SEQ, HEADS * HEAD_DIM)

def rms_scale(values_in):
    return values_in * lax.rsqrt(lax.optimization_barrier(jnp.mean(values_in * values_in, axis=-1, keepdims=True)) + EPS)

def layer(residual, params, starts, cos_table, sin_table):
    attn_gain, w_query, w_key, w_value, w_out, mlp_gain, w_gate, w_up, w_down = params
    head_width = D // GROUPS
    ff_width = FF // GROUPS
    group_shape = (SEQ, HEADS // GROUPS, HEAD_DIM)
    attn_in = low(rms_scale(residual) * attn_gain)
    query_parts, key_parts, value_parts = ([], [], [])
    for group in range(GROUPS):
        shared = low_back(attn_in)
        first_col = group * head_width
        last_col = first_col + head_width
        query_parts.append(low(rotate(low_back(mat_high(shared, w_query[:, first_col:last_col])).reshape(group_shape), cos_table, sin_table)))
        key_parts.append(low(rotate(low_back(mat_high(shared, w_key[:, first_col:last_col])).reshape(group_shape), cos_table, sin_table)))
        value_parts.append(low(low_back(mat_high(shared, w_value[:, first_col:last_col]))).reshape(group_shape))
    queries = jnp.concatenate(query_parts, axis=1)
    keys_rot = jnp.concatenate(key_parts, axis=1)
    values_in = jnp.concatenate(value_parts, axis=1)
    attended = low(low_back(attention(queries, keys_rot, values_in, starts)))
    attn_total = jnp.zeros((SEQ, D), jnp.float32)
    for group in range(GROUPS):
        first_col = group * head_width
        last_col = first_col + head_width
        attn_total = attn_total + low(mat_high(attended[:, first_col:last_col], w_out[first_col:last_col, :]))
    middle = residual + low_back(attn_total)
    mlp_in = low(rms_scale(middle) * mlp_gain)
    mlp_total = jnp.zeros((SEQ, D), jnp.float32)
    for group in range(GROUPS):
        shared = low_back(mlp_in)
        first_col = group * ff_width
        last_col = first_col + ff_width
        gate_pre = low_back(mat_high(shared, w_gate[:, first_col:last_col]))
        up_pre = low_back(mat_high(shared, w_up[:, first_col:last_col]))
        hidden = low(gate_pre * jax.nn.sigmoid(gate_pre) * up_pre)
        mlp_total = mlp_total + low(mat_high(hidden, w_down[first_col:last_col, :]))
    return middle + low_back(mlp_total)

def reference(hidden_in, out_grad, doc_lengths, attn_gain, w_query, w_key, w_value, w_out, mlp_gain, w_gate, w_up, w_down):
    params = tuple((weight.astype(jnp.float32) for weight in (attn_gain, w_query, w_key, w_value, w_out, mlp_gain, w_gate, w_up, w_down)))

    def per_row(totals, row_pack):
        input_row, grad_row, lengths = row_pack
        starts = doc_starts(lengths)
        cos_table, sin_table = rope_tables(starts)

        def forward(residual, weights):
            return layer(residual, weights, starts, cos_table, sin_table)
        result, pullback = jax.vjp(forward, input_row.astype(jnp.float32), params)
        grad_input, grad_params = pullback(grad_row.astype(jnp.float32))
        totals = tuple((summed + gradient for summed, gradient in zip(totals, grad_params)))
        return (totals, (result.astype(jnp.bfloat16), grad_input.astype(jnp.bfloat16)))
    zero_grads = tuple((jnp.zeros_like(weight) for weight in params))
    totals, (outputs, input_grads) = lax.scan(per_row, zero_grads, (hidden_in, out_grad, doc_lengths))
    return (outputs, input_grads, totals[0], totals[1], totals[2], totals[3], totals[4], totals[5], totals[6], totals[7], totals[8])
```

```python
import functools

import jax
import jax.numpy as jnp
from jax import lax
from jax.experimental import pallas as pl
from jax.experimental.pallas import tpu as pltpu
from jax.sharding import PartitionSpec as P

HEAD_DIM = 64
EPS = 1e-05
NEG = -1e30
ROPE_BASE = 130000.0
F32 = jnp.float32
BF16 = jnp.bfloat16
NN = (((1,), (0,)), ((), ()))
NT = (((1,), (1,)), ((), ()))
TN = (((0,), (0,)), ((), ()))
VMEM_LIMIT = 60 * 1024 * 1024
COST = 0.02


def dot(left, right, dims=NN):
    return lax.dot_general(left, right, dims, preferred_element_type=F32)


def params_for(**extra):
    return pltpu.CompilerParams(vmem_limit_bytes=VMEM_LIMIT, **extra)


def cost(flops, bytes_accessed, transcendentals):
    return pl.CostEstimate(
        flops=int(flops * COST),
        bytes_accessed=int(bytes_accessed * COST),
        transcendentals=int(transcendentals * COST),
    )


def vmem():
    return pl.BlockSpec(memory_space=pltpu.VMEM)


def smem():
    return pl.BlockSpec(memory_space=pltpu.SMEM)


def bits_of(count):
    return count.bit_length() - 1


def offset_at(place, count):
    top = bits_of(count) - 1
    return ((place << 1) & (count - 1)) | (place >> top)


def place_of(offset, count):
    top = bits_of(count) - 1
    return (offset >> 1) | ((offset & 1) << top)


def swap(block, bit):
    count = lax.axis_size("wide")
    return lax.ppermute(block, "wide", [(i, i ^ (1 << bit)) for i in range(count)])


def after(value, *others):
    return lax.optimization_barrier((value,) + others)[0] if others else value


class Slots:
    def __init__(self):
        self.now = []
        self.then = []

    def gate(self, value):
        return after(value, *self.now)

    def ends(self, value):
        self.then.append(value)
        return value

    def turn(self):
        self.now = self.then or self.now
        self.then = []

    def swap(self, block, bit, axis="wide", hold=True):
        count = lax.axis_size(axis)
        pairs = [(i, i ^ (1 << bit)) for i in range(count)]
        got = lax.ppermute(self.gate(block), axis, pairs)
        return self.ends(got) if hold else got


class Gather:
    def __init__(self, slots, block):
        self.slots = slots
        self.block = block
        chip_bits = bits_of(lax.axis_size("wide")) - 1
        self.plain = not (chip_bits == 2 and block.shape[0] % 32 == 0)
        if not self.plain:
            self.from_x = slots.swap(block, 1)
            self.from_y = slots.swap(block, 2)

    def far(self):
        if not self.plain:
            half = self.block.shape[0] // 2
            self.far_low = self.slots.swap(self.from_y[:half], 1)
            self.far_high = self.slots.swap(self.from_x[half:], 2)

    def core(self):
        if self.plain:
            pieces = [self.block]
            for bit in range(1, bits_of(lax.axis_size("wide"))):
                pieces = pieces + [self.slots.swap(piece, bit) for piece in pieces]
        else:
            pieces = [self.block, self.from_x, self.from_y, self.far_low, self.far_high]
        own = jnp.concatenate(pieces, axis=0)
        self.halves = [own, self.slots.swap(own, 0)]


class Scatter:
    def __init__(self, slots, lefts, rights, dims):
        self.slots = slots
        self.factors = (lefts, rights, dims)
        self.sent = self.product(1)

    def product(self, side, got=None):
        lefts, rights, dims = self.factors
        lefts = [self.slots.gate(lefts[0])] + list(lefts[1:])
        made = partial_sums(lefts, rights, dims, side, got)
        self.slots.ends(made[0] if isinstance(made, (list, tuple)) else made)
        return made

    def core(self):
        self.got = self.slots.swap(self.sent, 0)

    def even(self):
        self.kept = self.product(0, self.got)

    def near(self):
        if isinstance(self.kept, (tuple, list)):
            self.got_x = self.slots.swap(self.kept[2], 1)
            self.got_y = self.slots.swap(self.kept[3], 2)
            return
        kept = self.kept
        for bit in reversed(range(bits_of(lax.axis_size("wide")) - 1)):
            rows = kept.shape[0] // 2
            got = self.slots.swap(kept[rows:], bit + 1)
            kept = (kept[:rows].astype(F32) + got.astype(F32)).astype(BF16)
        self.total = kept.astype(F32)

    def last(self):
        if not isinstance(self.kept, (tuple, list)):
            return
        keep_low, keep_high = self.kept[:2]
        half = keep_low.shape[0] // 2
        far_low = (keep_low[half:].astype(F32) + self.got_x[half:].astype(F32)).astype(BF16)
        far_high = (keep_high[half:].astype(F32) + self.got_y[half:].astype(F32)).astype(BF16)
        low = self.slots.swap(far_low, 2)
        high = self.slots.swap(far_high, 1)
        low = keep_low[:half].astype(F32) + self.got_x[:half].astype(F32) + low.astype(F32)
        high = keep_high[:half].astype(F32) + self.got_y[:half].astype(F32) + high.astype(F32)
        self.total = jnp.concatenate([low, high], axis=0)


def partner_lanes(values, width):
    lanes = lax.broadcasted_iota(jnp.int32, values.shape, 1)
    first = (lanes % HEAD_DIM) < HEAD_DIM // 2
    half = HEAD_DIM // 2
    return jnp.where(first, pltpu.roll(values, width - half, 1), pltpu.roll(values, half, 1))


def wide_table(table, width):
    copies = width // table.shape[1]
    return jnp.concatenate([table] * copies, axis=1) if copies > 1 else table


def streaming_call(streams, body, ins, in_specs, outs, out_specs, name, flops, moved):
    seq = sum(piece.shape[0] for piece in streams[0])
    rows = min(512, streams[0][0].shape[0])
    steps = seq // rows
    plan = []
    for number, pieces in enumerate(streams):
        first = 0
        for piece in pieces:
            plan.append((number, first, piece.shape[0]))
            first += piece.shape[0]
    count, groups = len(plan), len(streams)

    def kernel(*refs):
        piece_refs, rest = refs[:count], refs[count:]
        middle_refs, buffers, sems = rest[: -groups - 1], rest[-groups - 1 : -1], rest[-1]
        step = pl.program_id(0)

        def copies(block, slot):
            found = []
            for ref, (number, first, size) in zip(piece_refs, plan):
                place = block * rows - first
                if 0 <= place < size:
                    source = ref.at[pl.ds(place, rows)]
                    found.append(
                        pltpu.make_async_copy(
                            source, buffers[number].at[slot], sems.at[number, slot]
                        )
                    )
            return found

        for block in range(steps):

            @pl.when(step == (0 if block == 0 else block - 1))
            def _():
                for copy in copies(block, block % 2):
                    copy.start()

        for block in range(steps):

            @pl.when(step == block)
            def _():
                for copy in copies(block, block % 2):
                    copy.wait()

        slot = lax.rem(step, 2)
        body(*[buffer.at[slot] for buffer in buffers], *middle_refs)

    return pl.pallas_call(
        kernel,
        out_shape=outs,
        grid=(steps,),
        in_specs=[pl.BlockSpec(memory_space=pl.ANY)] * count + in_specs(rows),
        out_specs=out_specs(rows),
        scratch_shapes=[pltpu.VMEM((2, rows, pieces[0].shape[1]), BF16) for pieces in streams]
        + [pltpu.SemaphoreType.DMA((groups, 2))],
        compiler_params=params_for(),
        cost_estimate=cost(
            flops=flops,
            bytes_accessed=moved + sum(2 * seq * pieces[0].shape[1] for pieces in streams),
            transcendentals=0,
        ),
        name=name,
    )(*[piece for pieces in streams for piece in pieces], *ins)


def resident(array):
    shape = array.shape
    return pl.BlockSpec(shape, lambda i: (0,) * len(shape), pipeline_mode=pl.Buffered(1))


def by_rows(rows, cols):
    return pl.BlockSpec((rows, cols), lambda i: (i, 0))


def project_qkv(tokens, weights, cos, sin):
    seq = sum(piece.shape[0] for piece in tokens)
    dim, cols = weights.shape
    width = cols // 3

    def body(x_ref, w_ref, cos_ref, sin_ref, out_ref):
        raw = dot(x_ref[...], w_ref[...])
        cos = wide_table(cos_ref[...], width)
        sin = wide_table(sin_ref[...], width)
        query = raw[:, :width]
        key = raw[:, width : 2 * width]
        query = (query * cos + partner_lanes(query, width) * sin) * (HEAD_DIM**-0.5)
        key = key * cos + partner_lanes(key, width) * sin
        out_ref[:, :width] = query.astype(BF16)
        out_ref[:, width : 2 * width] = key.astype(BF16)
        out_ref[:, 2 * width :] = raw[:, 2 * width :].astype(BF16)

    return streaming_call(
        [tokens],
        body,
        [weights, cos, sin],
        lambda rows: [resident(weights), by_rows(rows, cos.shape[1]), by_rows(rows, sin.shape[1])],
        jax.ShapeDtypeStruct((seq, cols), BF16),
        lambda rows: by_rows(rows, cols),
        "project_qkv",
        2 * seq * dim * cols,
        2 * (dim * cols + seq * cols),
    )


def pull_back_out(tokens, w_out):
    seq = sum(piece.shape[0] for piece in tokens)
    width, dim = w_out.shape

    def body(x_ref, w_ref, out_ref):
        out_ref[...] = dot(x_ref[...], w_ref[...], NT).astype(BF16)

    return streaming_call(
        [tokens],
        body,
        [w_out],
        lambda rows: [resident(w_out)],
        jax.ShapeDtypeStruct((seq, width), BF16),
        lambda rows: by_rows(rows, width),
        "pull_back_out",
        2 * seq * dim * width,
        2 * (dim * width + seq * width),
    )


def mlp_body(x_ref, gy_ref, gu_ref, down_ref, hid_ref, dgu_ref):
    cols = hid_ref.shape[1]
    both = dot(x_ref[...], gu_ref[...])
    d_hid = dot(gy_ref[...], down_ref[...], NT)
    gp = both[:, :cols]
    up = both[:, cols:]
    sig = jax.nn.sigmoid(gp)
    silu = gp * sig
    hid_ref[...] = (silu * up).astype(BF16)
    dgu_ref[:, :cols] = (d_hid * up * sig * (1.0 + gp * (1.0 - sig))).astype(BF16)
    dgu_ref[:, cols:] = (d_hid * silu).astype(BF16)


def mlp_products(tokens, gy, w_gu, w_down):
    seq = sum(piece.shape[0] for piece in tokens)
    cols, dim = w_down.shape
    return streaming_call(
        [tokens, gy],
        mlp_body,
        [w_gu, w_down],
        lambda rows: [resident(w_gu), resident(w_down)],
        [jax.ShapeDtypeStruct((seq, cols), BF16), jax.ShapeDtypeStruct((seq, 2 * cols), BF16)],
        lambda rows: [by_rows(rows, cols), by_rows(rows, 2 * cols)],
        "mlp_products",
        6 * seq * dim * cols,
        2 * (3 * dim * cols + 3 * seq * cols),
    )


def partial_sums(lefts, rights, dims, side, got=None):
    seq = lefts[0].shape[0]
    dim = rights[0].shape[1] if dims == NN else rights[0].shape[0]
    rows = seq // 2
    count = len(lefts)
    wide = lax.axis_size("wide")
    chunk = seq // wide
    split = got is not None and bits_of(wide) == 3 and chunk % 32 == 0
    block = chunk if split else min(512, rows)
    steps = rows // block
    half = block // 2

    def kernel(*refs):
        total = None
        for left, right in zip(refs[:count], refs[count : 2 * count]):
            term = dot(left[...], right[...], dims)
            total = term if total is None else total + term
        if got is None:
            refs[-1][...] = total.astype(BF16)
            return
        total = total + refs[2 * count][...].astype(F32)
        if not split:
            refs[-1][...] = total.astype(BF16)
            return
        keep_low, keep_high, send_x, send_y = refs[-4:]
        step = pl.program_id(0)
        low = total[:half].astype(BF16)
        high = total[half:].astype(BF16)

        @pl.when(step % 2 == 0)
        def _():
            keep_low[...] = low

        @pl.when(step % 2 == 1)
        def _():
            send_x[...] = low

        @pl.when(step < 2)
        def _():
            keep_high[...] = high

        @pl.when(step >= 2)
        def _():
            send_y[...] = high

    in_specs = [
        pl.BlockSpec((block, left.shape[1]), lambda i: (side * steps + i, 0)) for left in lefts
    ] + [resident(right) for right in rights]
    ins = list(lefts) + list(rights)
    if got is not None:
        in_specs.append(by_rows(block, dim))
        ins.append(got)
    if split:
        out_shape = [jax.ShapeDtypeStruct((2 * half, dim), BF16)] * 4
        out_specs = [
            pl.BlockSpec((half, dim), lambda i: (i // 2, 0)),
            pl.BlockSpec((half, dim), lambda i: (jnp.minimum(i, 1), 0)),
            pl.BlockSpec((half, dim), lambda i: (i // 2, 0)),
            pl.BlockSpec((half, dim), lambda i: (jnp.maximum(i - 2, 0), 0)),
        ]
    else:
        out_shape = jax.ShapeDtypeStruct((rows, dim), BF16)
        out_specs = by_rows(block, dim)
    depth = sum(left.shape[1] for left in lefts)
    return pl.pallas_call(
        kernel,
        out_shape=out_shape,
        grid=(steps,),
        in_specs=in_specs,
        out_specs=out_specs,
        compiler_params=params_for(),
        cost_estimate=cost(
            flops=2 * rows * depth * dim,
            bytes_accessed=2 * (rows * depth + depth * dim + 2 * rows * dim),
            transcendentals=0,
        ),
        name="partial_sums",
    )(*ins)


def whole_sums(lefts, rights, dims, place):
    seq = lefts[0].shape[0]
    dim = rights[0].shape[1] if dims == NN else rights[0].shape[0]
    chunks = place.shape[0]
    block = seq // chunks
    count = len(lefts)

    def kernel(place_ref, *refs):
        total = None
        for left, right in zip(refs[:count], refs[count : 2 * count]):
            term = dot(left[...], right[...], dims)
            total = term if total is None else total + term
        refs[-1][...] = total.astype(BF16)

    def whole(array):
        return pl.BlockSpec(array.shape, lambda i, at: (0, 0), pipeline_mode=pl.Buffered(1))

    depth = sum(left.shape[1] for left in lefts)
    return pl.pallas_call(
        kernel,
        out_shape=jax.ShapeDtypeStruct((seq, dim), BF16),
        grid_spec=pltpu.PrefetchScalarGridSpec(
            num_scalar_prefetch=1,
            grid=(chunks,),
            in_specs=[
                pl.BlockSpec((block, left.shape[1]), lambda i, at: (at[i], 0)) for left in lefts
            ]
            + [whole(right) for right in rights],
            out_specs=pl.BlockSpec((block, dim), lambda i, at: (i, 0)),
        ),
        compiler_params=params_for(),
        cost_estimate=cost(
            flops=2 * seq * depth * dim,
            bytes_accessed=2 * (seq * depth + depth * dim + seq * dim),
            transcendentals=0,
        ),
        name="whole_sums",
    )(place, *lefts, *rights)


def halves(array):
    if isinstance(array, (list, tuple)):
        return [(half, 0) for half in array]
    return [(array, 0), (array, 1)]


def weight_grad(lefts, rights, seq):
    seq //= 2
    lefts = [pair for left in lefts for pair in halves(left)]
    rights = [pair for right in rights for pair in halves(right)]
    height = lefts[0][0].shape[1]
    cols = rights[0][0].shape[1]
    tall = min(512 if height < 1024 else 256, height)
    wide = min(1024, cols)
    count = len(lefts)

    def kernel(*refs):
        total = None
        for left, right in zip(refs[:count], refs[count : 2 * count]):
            term = dot(left[...], right[...], TN)
            total = term if total is None else total + term
        refs[-1][...] = total.astype(BF16)

    return pl.pallas_call(
        kernel,
        out_shape=jax.ShapeDtypeStruct((height, cols), BF16),
        grid=(cols // wide, height // tall),
        in_specs=[pl.BlockSpec((seq, tall), lambda n, m, p=p: (p, m)) for _, p in lefts]
        + [pl.BlockSpec((seq, wide), lambda n, m, p=p: (p, n)) for _, p in rights],
        out_specs=pl.BlockSpec((tall, wide), lambda n, m: (m, n)),
        compiler_params=params_for(),
        cost_estimate=cost(
            flops=2 * seq * height * cols * count,
            bytes_accessed=2 * count * (seq * height * (cols // wide) + seq * cols),
            transcendentals=0,
        ),
        name="weight_grad",
    )(*[a for a, _ in lefts], *[a for a, _ in rights])


def head_stack(block, heads):
    lanes = lax.broadcasted_iota(jnp.int32, block.shape, 1) // HEAD_DIM
    zero = jnp.zeros_like(block)
    return jnp.concatenate([jnp.where(lanes == h, block, zero) for h in range(heads)], axis=0)


def block_mask(first_key, first_query, begins, size):
    keys = first_key + lax.broadcasted_iota(jnp.int32, (size, size), 0)
    queries = first_query + lax.broadcasted_iota(jnp.int32, (size, size), 1)
    return (keys <= queries) & (keys >= begins)


def forward_kernel(heads, blocks, size, low_ref, place_ref, begins_ref, qkv_ref, att_ref, lse_ref, vt_ref):
    width = heads * HEAD_DIM

    def spin(b, carry):
        rows = pl.ds(pl.multiple_of(place_ref[b] * size, size), size)
        vt_ref[b] = qkv_ref[rows, 2 * width :].astype(F32).T.astype(BF16)
        return carry

    lax.fori_loop(0, blocks, spin, 0)

    def one_query_block(i, carry):
        rows = pl.ds(pl.multiple_of(place_ref[i] * size, size), size)
        stack = head_stack(qkv_ref[rows, :width], heads)
        begins = begins_ref[i]

        def one_key_block(j, state):
            maxes, totals, sums = state
            keys = pl.ds(pl.multiple_of(place_ref[j] * size, size), size)
            scores = dot(qkv_ref[keys, width : 2 * width], stack, NT)
            allowed = block_mask(j * size, i * size, begins, size)
            new_maxes, new_totals, new_sums = [], [], []
            for h in range(heads):
                part = jnp.where(allowed, scores[:, h * size : (h + 1) * size], NEG)
                peak = jnp.maximum(maxes[h], jnp.max(part, axis=0, keepdims=True))
                fade = jnp.exp(maxes[h] - peak)
                probs = jnp.exp(part - peak)
                new_maxes.append(peak)
                new_totals.append(totals[h] * fade + jnp.sum(probs, axis=0, keepdims=True))
                values_t = vt_ref[j, h * HEAD_DIM : (h + 1) * HEAD_DIM, :]
                new_sums.append(sums[h] * fade + dot(values_t, probs.astype(BF16)))
            return (tuple(new_maxes), tuple(new_totals), tuple(new_sums))

        start = (
            tuple(jnp.full((1, size), NEG, F32) for _ in range(heads)),
            tuple(jnp.zeros((1, size), F32) for _ in range(heads)),
            tuple(jnp.zeros((HEAD_DIM, size), F32) for _ in range(heads)),
        )
        maxes, totals, sums = lax.fori_loop(low_ref[i], i + 1, one_key_block, start)
        outs = jnp.concatenate([sums[h] / totals[h] for h in range(heads)], axis=0)
        att_ref[rows, :] = outs.T.astype(BF16)
        for h in range(heads):
            lse_ref[i, h : h + 1, :] = maxes[h] + jnp.log(totals[h])
        return carry

    lax.fori_loop(0, blocks, one_query_block, 0)


def attend_forward(qkv, low, place, begins, heads):
    seq = qkv.shape[0]
    blocks, _, size = begins.shape
    width = heads * HEAD_DIM
    pairs = seq * seq // 3
    return pl.pallas_call(
        functools.partial(forward_kernel, heads, blocks, size),
        out_shape=(
            jax.ShapeDtypeStruct((seq, width), BF16),
            jax.ShapeDtypeStruct((blocks, heads, size), F32),
        ),
        in_specs=[smem(), smem(), vmem(), vmem()],
        out_specs=(vmem(), vmem()),
        scratch_shapes=[pltpu.VMEM((blocks, width, size), BF16)],
        compiler_params=params_for(),
        cost_estimate=cost(
            flops=16 * pairs * width,
            bytes_accessed=2 * seq * width * 4,
            transcendentals=pairs * heads,
        ),
        name="attend_forward",
    )(low, place, begins, qkv)


def backward_kernel(
    heads,
    blocks,
    size,
    low_ref,
    place_ref,
    begins_ref,
    qkv_ref,
    att_ref,
    grad_ref,
    lse_ref,
    cos_ref,
    sin_ref,
    out_ref,
    kt_ref,
    dk_ref,
    dv_ref,
):
    width = heads * HEAD_DIM
    scale = HEAD_DIM**-0.5

    def spin(b, carry):
        rows = pl.ds(pl.multiple_of(place_ref[b] * size, size), size)
        kt_ref[b] = qkv_ref[rows, width : 2 * width].astype(F32).T.astype(BF16)
        dk_ref[b] = jnp.zeros((size, width), F32)
        dv_ref[b] = jnp.zeros((size, width), F32)
        return carry

    lax.fori_loop(0, blocks, spin, 0)

    def unrotate(values, rows):
        cos = wide_table(cos_ref[rows, :], width)
        sin = wide_table(sin_ref[rows, :], width)
        return values * cos - partner_lanes(values, width) * sin

    def one_query_block(i, carry):
        rows = pl.ds(pl.multiple_of(place_ref[i] * size, size), size)
        q_stack = head_stack(qkv_ref[rows, :width], heads)
        grad = grad_ref[rows, :]
        g_stack = head_stack(grad, heads)
        product = (grad.astype(F32) * att_ref[rows, :].astype(F32)).T
        deltas = [
            jnp.sum(product[h * HEAD_DIM : (h + 1) * HEAD_DIM], axis=0, keepdims=True)
            for h in range(heads)
        ]
        begins = begins_ref[i]

        def one_key_block(j, sums):
            keys = pl.ds(pl.multiple_of(place_ref[j] * size, size), size)
            scores = dot(qkv_ref[keys, width : 2 * width], q_stack, NT)
            grads = dot(qkv_ref[keys, 2 * width :], g_stack, NT)
            allowed = block_mask(j * size, i * size, begins, size)
            all_probs, all_ds, new_sums = [], [], []
            for h in range(heads):
                span = slice(h * size, (h + 1) * size)
                part = jnp.where(allowed, scores[:, span] - lse_ref[i, h : h + 1, :], NEG)
                probs = jnp.exp(part)
                d_scores = (probs * (grads[:, span] - deltas[h])).astype(BF16)
                all_probs.append(probs.astype(BF16))
                all_ds.append(d_scores)
                keys_t = kt_ref[j, h * HEAD_DIM : (h + 1) * HEAD_DIM, :]
                new_sums.append(sums[h] + dot(keys_t, d_scores))
            dv_ref[j] += dot(jnp.concatenate(all_probs, axis=1), g_stack)
            dk_ref[j] += dot(jnp.concatenate(all_ds, axis=1), q_stack)
            return tuple(new_sums)

        start = tuple(jnp.zeros((HEAD_DIM, size), F32) for _ in range(heads))
        sums = lax.fori_loop(low_ref[i], i + 1, one_key_block, start)
        query_grad = jnp.concatenate(sums, axis=0).T * scale
        out_ref[rows, :width] = unrotate(query_grad, rows).astype(BF16)
        return carry

    lax.fori_loop(0, blocks, one_query_block, 0)

    def finish(b, carry):
        rows = pl.ds(pl.multiple_of(place_ref[b] * size, size), size)
        out_ref[rows, width : 2 * width] = unrotate(dk_ref[b], rows).astype(BF16)
        out_ref[rows, 2 * width :] = dv_ref[b].astype(BF16)
        return carry

    lax.fori_loop(0, blocks, finish, 0)


def attend_backward(qkv, att, grad, lse, low, place, begins, cos, sin, heads):
    seq = qkv.shape[0]
    blocks, _, size = begins.shape
    width = heads * HEAD_DIM
    pairs = seq * seq // 3
    return pl.pallas_call(
        functools.partial(backward_kernel, heads, blocks, size),
        out_shape=jax.ShapeDtypeStruct((seq, 3 * width), BF16),
        in_specs=[smem(), smem()] + [vmem()] * 7,
        out_specs=vmem(),
        scratch_shapes=[
            pltpu.VMEM((blocks, width, size), BF16),
            pltpu.VMEM((blocks, size, width), F32),
            pltpu.VMEM((blocks, size, width), F32),
        ],
        compiler_params=params_for(),
        cost_estimate=cost(
            flops=40 * pairs * width,
            bytes_accessed=2 * seq * width * 10,
            transcendentals=pairs * heads,
        ),
        name="attend_backward",
    )(low, place, begins, qkv, att, grad, lse, cos, sin)


def row_facts(lengths, seq):
    wide = lax.axis_size("wide")
    me = lax.axis_index("wide")
    chunk = seq // wide
    docs = lengths.shape[0]
    upto = jnp.arange(docs)[:, None] <= jnp.arange(docs)[None, :]
    ends = jnp.sum(jnp.where(upto, lengths[:, None], 0), axis=0).astype(jnp.int32)

    def starts_of(tokens):
        before = jnp.where(ends[None, :] <= tokens[:, None], ends[None, :], jnp.int32(0))
        return jnp.max(before, axis=1)

    tokens = jnp.arange(seq, dtype=jnp.int32)
    begins = starts_of(tokens).reshape(wide, 1, chunk)
    low = begins[:, 0, 0] // chunk
    index = jnp.arange(wide, dtype=jnp.int32)
    place = place_of(index ^ me, wide)
    owner = me ^ offset_at(index, wide)
    here = (owner[:, None] * chunk + jnp.arange(chunk, dtype=jnp.int32)[None, :]).reshape(seq)
    position = (here - starts_of(here)).astype(F32)
    half_dim = HEAD_DIM // 2
    inverse = ROPE_BASE ** (-(jnp.arange(half_dim, dtype=F32) * 2.0) / HEAD_DIM)
    angles = position[:, None] * inverse[None, :]
    cos = jnp.cos(angles)
    sin = jnp.sin(angles)
    cos = jnp.concatenate([cos, cos, cos, cos], axis=1)
    sin = jnp.concatenate([-sin, sin, -sin, sin], axis=1)
    return low, place, begins, cos, sin


def norm_scale(values):
    return lax.rsqrt(jnp.mean(values * values, axis=-1, keepdims=True) + EPS)


def per_device(
    hidden_in,
    out_grad,
    doc_lengths,
    attn_gain,
    w_query,
    w_key,
    w_value,
    w_out,
    mlp_gain,
    w_gate,
    w_up,
    w_down,
):
    narrow = lax.axis_size("narrow")
    wide = lax.axis_size("wide")
    here = lax.axis_index("narrow")
    rows_here, chunk, dim = hidden_in.shape
    seq = chunk * wide
    width = w_query.shape[1]
    heads = width // HEAD_DIM

    def fetch(weight, axis):
        return lax.all_gather(weight, "narrow", axis=axis, tiled=True)

    gains = jnp.stack([attn_gain, mlp_gain])
    turned = [gains]
    for step in range(1, narrow):
        turned.append(
            lax.ppermute(gains, "narrow", [((i + step) % narrow, i) for i in range(narrow)])
        )
    order = (jnp.arange(narrow) - here) % narrow
    gains = jnp.take(jnp.stack(turned), order, axis=0)
    gains = jnp.swapaxes(gains, 0, 1).reshape(2, dim).astype(F32)
    attn_scale = gains[0]
    mlp_scale = gains[1]

    slots = Slots()
    gate, ends, turn = slots.gate, slots.ends, slots.turn
    hidden = w_gate.shape[1]
    cut = hidden // 2
    spans = [slice(0, cut), slice(cut, hidden)]
    w_qkv = fetch(jnp.concatenate([w_query, w_key, w_value], axis=1), 0)
    full_out = fetch(w_out, 1)
    full_gu, full_down = [], []
    for span in spans:
        full_gu.append(fetch(jnp.concatenate([w_gate[:, span], w_up[:, span]], axis=1), 0))
        full_down.append(fetch(w_down[span], 1))

    rows = range(rows_here)
    last = rows_here - 1
    facts = [row_facts(doc_lengths[r], seq) for r in rows]
    residual = [hidden_in[r].astype(F32) for r in rows]
    inv_first = [norm_scale(residual[r]) for r in rows]
    normed = [residual[r] * inv_first[r] for r in rows]
    scaled_in = [(normed[r] * attn_scale).astype(BF16) for r in rows]

    attn_in, gy, mlp_in, branch = {}, {}, {}, {}
    qkv, att, lse, middle, inv_second, normed_mid = ({} for _ in range(6))
    grad_middle, gain_mlp, gain_attn, outputs, in_grads, d_qkv = ({} for _ in range(6))
    hid = {r: [] for r in rows}
    d_gu = {r: [] for r in rows}

    def first_of(halves):
        return [gate(halves[0])] + list(halves[1:])

    def project(r):
        _, _, _, cos, sin = facts[r]
        qkv[r] = ends(project_qkv(first_of(attn_in[r].halves), w_qkv, cos, sin))

    def attend(r):
        low, place, begins, _, _ = facts[r]
        att[r], lse[r] = attend_forward(gate(qkv[r]), low, place, begins, heads)
        ends(att[r])

    def spread(lefts, rights, dims):
        return Scatter(slots, lefts, rights, dims)

    def after_attention(r, total):
        total = gate(total)
        middle[r] = residual[r] + total
        inv_second[r] = norm_scale(middle[r])
        normed_mid[r] = middle[r] * inv_second[r]
        mlp_in[r] = Gather(slots, (normed_mid[r] * mlp_scale).astype(BF16))

    def mlp(r, part):
        one, two = mlp_products(
            first_of(mlp_in[r].halves), gy[r].halves, full_gu[part], full_down[part]
        )
        ends(one)
        hid[r].append(one)
        d_gu[r].append(two)

    def after_mlp(r, total):
        total = gate(total)
        gain_mlp[r] = jnp.sum(total * normed_mid[r], axis=0)
        scaled = total * mlp_scale
        grad_middle[r] = out_grad[r].astype(F32) + inv_second[r] * (
            scaled - normed_mid[r] * jnp.mean(scaled * normed_mid[r], axis=-1, keepdims=True)
        )
        branch[r] = Gather(slots, grad_middle[r].astype(BF16))

    def back_attention(r):
        low, place, begins, cos, sin = facts[r]
        grad_att = pull_back_out(first_of(branch[r].halves), full_out)
        d_qkv[r] = ends(
            attend_backward(
                qkv[r], att[r], grad_att, lse[r], low, place, begins, cos, sin, heads
            )
        )

    def after_back(r, total):
        total = gate(total)
        gain_attn[r] = jnp.sum(total * normed[r], axis=0)
        scaled = total * attn_scale
        in_grads[r] = (
            grad_middle[r]
            + inv_first[r]
            * (scaled - normed[r] * jnp.mean(scaled * normed[r], axis=-1, keepdims=True))
        ).astype(BF16)

    def grad_of(lefts, rights, axis):
        lefts = [lefts[r] for r in rows]
        lefts[0] = first_of(lefts[0]) if isinstance(lefts[0], list) else gate(lefts[0])
        grad = ends(weight_grad(lefts, [rights[r] for r in rows], seq))
        return lax.psum_scatter(grad, "narrow", scatter_dimension=axis, tiled=True).astype(F32)

    def both(table):
        return [table[r] for r in rows]

    def halves_of(table):
        return {r: table[r].halves for r in rows}

    def part_of(table, part):
        return {r: table[r][part] for r in rows}

    sums, down, grad_gu, grad_down = {}, {}, [None, None], [None, None]

    def out_sum(r):
        sums[r] = spread([att[r]], [full_out], NN)

    def mlp_sum(r):
        whole = ends(whole_sums(first_of(d_gu[r]), full_gu, NT, facts[r][1]))
        sums[r] = lax.psum_scatter(whole, "wide", scatter_dimension=0, tiled=True).astype(F32)

    def back_sum(r):
        sums[r] = spread([d_qkv[r]], [w_qkv], NT)

    def down_sum(r):
        down[r] = spread(hid[r], full_down, NN)

    def gu_grad(part):
        grad_gu[part] = grad_of(halves_of(mlp_in), part_of(d_gu, part), 0)

    def down_grad(part):
        grad_down[part] = grad_of(part_of(hid, part), halves_of(gy), 1)

    one, two = 0, last
    attn_in[one] = Gather(slots, scaled_in[one])
    turn()
    attn_in[one].far()
    turn()
    attn_in[one].core()
    ends(w_qkv)
    turn()
    project(one)
    attn_in[two] = Gather(slots, scaled_in[two])
    ends(full_out)
    turn()
    attend(one)
    attn_in[two].far()
    turn()
    out_sum(one)
    attn_in[two].core()
    turn()
    project(two)
    sums[one].core()
    gy[one] = Gather(slots, out_grad[one])
    ends(full_down[0])
    turn()
    sums[one].even()
    gy[one].far()
    turn()
    attend(two)
    sums[one].near()
    gy[one].core()
    turn()
    out_sum(two)
    sums[one].last()
    ends(full_gu[0])
    turn()
    after_attention(one, sums[one].total)
    sums[two].core()
    turn()
    sums[two].even()
    mlp_in[one].far()
    turn()
    mlp_in[one].core()
    sums[two].near()
    ends(full_down[1])
    turn()
    mlp(one, 0)
    sums[two].last()
    gy[two] = Gather(slots, out_grad[two])
    turn()
    after_attention(two, sums[two].total)
    gy[two].far()
    turn()
    mlp_in[two].far()
    gy[two].core()
    ends(full_gu[1])
    turn()
    mlp(one, 1)
    mlp_in[two].core()
    turn()
    mlp_sum(one)
    turn()
    mlp(two, 0)
    turn()
    mlp(two, 1)
    turn()
    mlp_sum(two)
    turn()
    gu_grad(0)
    after_mlp(one, sums[one])
    turn()
    gu_grad(1)
    branch[one].far()
    turn()
    down_sum(one)
    down_sum(two)
    branch[one].core()
    turn()
    back_attention(one)
    after_mlp(two, sums[two])
    down[one].core()
    down[two].core()
    turn()
    back_sum(one)
    down[one].even()
    branch[two].far()
    turn()
    down_grad(0)
    branch[two].core()
    sums[one].core()
    down[one].near()
    turn()
    sums[one].even()
    down[two].even()
    down[one].last()
    turn()
    back_attention(two)
    sums[one].near()
    turn()
    back_sum(two)
    sums[one].last()
    turn()
    grad_qkv = grad_of(halves_of(attn_in), d_qkv, 0)
    sums[two].core()
    down[two].near()
    turn()
    sums[two].even()
    down[two].last()
    turn()
    grad_out = grad_of(att, halves_of(branch), 1)
    down_grad(1)
    sums[two].near()
    turn()
    sums[two].last()
    turn()
    for r in rows:
        outputs[r] = (middle[r] + down[r].total).astype(BF16)
        after_back(r, sums[r].total)

    def spread_gain(parts):
        total = sum(parts[1:], parts[0])
        for axis in ("narrow", "wide"):
            count = lax.axis_size(axis)
            me = lax.axis_index(axis)
            for bit in reversed(range(bits_of(count))):
                size = total.shape[0] // 2
                mine = (me >> bit) & 1
                sent = lax.dynamic_slice_in_dim(total, (1 - mine) * size, size)
                kept = lax.dynamic_slice_in_dim(total, mine * size, size)
                pairs = [(i, i ^ (1 << bit)) for i in range(count)]
                total = kept + lax.ppermute(sent, axis, pairs)
        return total

    grad_gate = [piece[:, :cut] for piece in grad_gu]
    grad_up = [piece[:, cut:] for piece in grad_gu]
    return (
        jnp.stack(both(outputs)),
        jnp.stack(both(in_grads)),
        spread_gain(both(gain_attn)),
        grad_qkv[:, :width],
        grad_qkv[:, width : 2 * width],
        grad_qkv[:, 2 * width :],
        grad_out,
        spread_gain(both(gain_mlp)),
        jnp.concatenate(grad_gate, axis=1),
        jnp.concatenate(grad_up, axis=1),
        jnp.concatenate(grad_down, axis=0),
    )


def solution(mesh):
    in_specs = (
        P("narrow", "wide", None),
        P("narrow", "wide", None),
        P("narrow", None),
        P("narrow"),
        P("narrow", "wide"),
        P("narrow", "wide"),
        P("narrow", "wide"),
        P("wide", "narrow"),
        P("narrow"),
        P("narrow", "wide"),
        P("narrow", "wide"),
        P("wide", "narrow"),
    )
    out_specs = (
        P("narrow", "wide", None),
        P("narrow", "wide", None),
        P(("narrow", "wide")),
        P("narrow", "wide"),
        P("narrow", "wide"),
        P("narrow", "wide"),
        P("wide", "narrow"),
        P(("narrow", "wide")),
        P("narrow", "wide"),
        P("narrow", "wide"),
        P("wide", "narrow"),
    )
    return jax.shard_map(
        per_device, mesh=mesh, in_specs=in_specs, out_specs=out_specs, check_vma=False
    )
```

```python
import functools

import jax
import jax.numpy as jnp
from jax import lax
from jax.experimental import pallas as pl
from jax.experimental.pallas import tpu as pltpu
from jax.sharding import PartitionSpec as P

HEAD_DIM = 64
EPS = 1e-05
NEG = -1e30
ROPE_BASE = 130000.0
F32 = jnp.float32
BF16 = jnp.bfloat16
NN = (((1,), (0,)), ((), ()))
NT = (((1,), (1,)), ((), ()))
TN = (((0,), (0,)), ((), ()))
VMEM_LIMIT = 60 * 1024 * 1024
COST = 0.02


def dot(left, right, dims=NN):
    return lax.dot_general(left, right, dims, preferred_element_type=F32)


def params_for(**extra):
    return pltpu.CompilerParams(vmem_limit_bytes=VMEM_LIMIT, **extra)


def cost(flops, bytes_accessed, transcendentals):
    return pl.CostEstimate(
        flops=int(flops * COST),
        bytes_accessed=int(bytes_accessed * COST),
        transcendentals=int(transcendentals * COST),
    )


def vmem():
    return pl.BlockSpec(memory_space=pltpu.VMEM)


def smem():
    return pl.BlockSpec(memory_space=pltpu.SMEM)


def bits_of(count):
    return count.bit_length() - 1


def offset_at(place, count):
    top = bits_of(count) - 1
    return ((place << 1) & (count - 1)) | (place >> top)


def place_of(offset, count):
    top = bits_of(count) - 1
    return (offset >> 1) | ((offset & 1) << top)


def swap(block, bit):
    count = lax.axis_size("wide")
    return lax.ppermute(block, "wide", [(i, i ^ (1 << bit)) for i in range(count)])


def after(value, *others):
    return lax.optimization_barrier((value,) + others)[0] if others else value


class Slots:
    def __init__(self):
        self.now = []
        self.then = []
        self.waiting = []

    def later(self, action):
        self.waiting.append(action)

    def gate(self, value):
        return after(value, *self.now)

    def ends(self, value):
        self.then.append(value)
        return value

    def turn(self):
        self.now = self.then or self.now
        self.then = []
        waiting, self.waiting = self.waiting, []
        for action in waiting:
            action()

    def swap(self, block, bit, axis="wide", hold=True):
        count = lax.axis_size(axis)
        pairs = [(i, i ^ (1 << bit)) for i in range(count)]
        got = lax.ppermute(self.gate(block), axis, pairs)
        return self.ends(got) if hold else got


class Gather:
    def __init__(self, slots, block):
        self.slots = slots
        self.block = block
        chip_bits = bits_of(lax.axis_size("wide")) - 1
        self.plain = not (chip_bits == 2 and block.shape[0] % 32 == 0)
        if not self.plain:
            self.from_x = slots.swap(block, 1)
            self.from_y = slots.swap(block, 2)

    def far(self):
        if not self.plain:
            half = self.block.shape[0] // 2
            self.far_low = self.slots.swap(self.from_y[:half], 1)
            self.far_high = self.slots.swap(self.from_x[half:], 2)

    def core(self):
        if self.plain:
            pieces = [self.block]
            for bit in range(1, bits_of(lax.axis_size("wide"))):
                pieces = pieces + [self.slots.swap(piece, bit) for piece in pieces]
        else:
            pieces = [self.block, self.from_x, self.from_y, self.far_low, self.far_high]
        own = jnp.concatenate(pieces, axis=0)
        self.halves = [own, self.slots.swap(own, 0)]


class Offloaded:
    def __init__(self, slots, block):
        self.slots = slots
        count = lax.axis_size("wide")
        groups = [list(range(core, count, 2)) for core in range(2)]
        self.chips = lax.all_gather(
            slots.gate(block), "wide", axis_index_groups=groups, axis=0, tiled=True
        )

    def core(self):
        chips = lax.axis_size("wide") // 2
        rows = self.chips.shape[0] // chips
        here = lax.axis_index("wide") // 2
        own = jnp.concatenate(
            [
                lax.dynamic_slice_in_dim(self.chips, (here ^ chip) * rows, rows)
                for chip in range(chips)
            ],
            axis=0,
        )
        self.halves = [own, self.slots.swap(own, 0)]


class Scatter:
    def __init__(self, slots, lefts, rights):
        self.slots = slots
        self.factors = (lefts, rights)
        self.sent = self.product(1)

    def product(self, side, got=None):
        lefts, rights = self.factors
        lefts = [self.slots.gate(lefts[0])] + list(lefts[1:])
        made = partial_sums(lefts, rights, side, got)
        self.slots.ends(made[0] if isinstance(made, (list, tuple)) else made)
        return made

    def core(self):
        self.got = self.slots.swap(self.sent, 0)

    def even(self):
        self.kept = self.product(0, self.got)

    def near(self):
        if isinstance(self.kept, (tuple, list)):
            self.got_x = self.slots.swap(self.kept[2], 1)
            self.got_y = self.slots.swap(self.kept[3], 2)
            return
        kept = self.kept
        for bit in reversed(range(bits_of(lax.axis_size("wide")) - 1)):
            rows = kept.shape[0] // 2
            got = self.slots.swap(kept[rows:], bit + 1)
            kept = (kept[:rows].astype(F32) + got.astype(F32)).astype(BF16)
        self.total = kept.astype(F32)

    def last(self, hold=True):
        if not isinstance(self.kept, (tuple, list)):
            return
        keep_low, keep_high = self.kept[:2]
        half = keep_low.shape[0] // 2
        far_low = (keep_low[half:].astype(F32) + self.got_x[half:].astype(F32)).astype(BF16)
        far_high = (keep_high[half:].astype(F32) + self.got_y[half:].astype(F32)).astype(BF16)
        low = self.slots.swap(far_low, 2, hold=hold)
        high = self.slots.swap(far_high, 1, hold=hold)
        low = keep_low[:half].astype(F32) + self.got_x[:half].astype(F32) + low.astype(F32)
        high = keep_high[:half].astype(F32) + self.got_y[:half].astype(F32) + high.astype(F32)
        self.total = jnp.concatenate([low, high], axis=0)


def partner_lanes(values, width):
    lanes = lax.broadcasted_iota(jnp.int32, values.shape, 1)
    first = (lanes % HEAD_DIM) < HEAD_DIM // 2
    half = HEAD_DIM // 2
    return jnp.where(first, pltpu.roll(values, width - half, 1), pltpu.roll(values, half, 1))


def wide_table(table, width):
    copies = width // table.shape[1]
    return jnp.concatenate([table] * copies, axis=1) if copies > 1 else table


def streaming_call(streams, body, ins, in_specs, outs, out_specs, name, flops, moved):
    seq = sum(piece.shape[0] for piece in streams[0])
    rows = min(512, streams[0][0].shape[0])
    steps = seq // rows
    plan = []
    for number, pieces in enumerate(streams):
        first = 0
        for piece in pieces:
            plan.append((number, first, piece.shape[0]))
            first += piece.shape[0]
    count, groups = len(plan), len(streams)

    def kernel(*refs):
        piece_refs, rest = refs[:count], refs[count:]
        middle_refs, buffers, sems = rest[: -groups - 1], rest[-groups - 1 : -1], rest[-1]
        step = pl.program_id(0)

        def copies(block, slot):
            found = []
            for ref, (number, first, size) in zip(piece_refs, plan):
                place = block * rows - first
                if 0 <= place < size:
                    source = ref.at[pl.ds(place, rows)]
                    found.append(
                        pltpu.make_async_copy(
                            source, buffers[number].at[slot], sems.at[number, slot]
                        )
                    )
            return found

        for block in range(steps):

            @pl.when(step == (0 if block == 0 else block - 1))
            def _():
                for copy in copies(block, block % 2):
                    copy.start()

        for block in range(steps):

            @pl.when(step == block)
            def _():
                for copy in copies(block, block % 2):
                    copy.wait()

        slot = lax.rem(step, 2)
        body(*[buffer.at[slot] for buffer in buffers], *middle_refs)

    return pl.pallas_call(
        kernel,
        out_shape=outs,
        grid=(steps,),
        in_specs=[pl.BlockSpec(memory_space=pl.ANY)] * count + in_specs(rows),
        out_specs=out_specs(rows),
        scratch_shapes=[pltpu.VMEM((2, rows, pieces[0].shape[1]), BF16) for pieces in streams]
        + [pltpu.SemaphoreType.DMA((groups, 2))],
        compiler_params=params_for(),
        cost_estimate=cost(
            flops=flops,
            bytes_accessed=moved + sum(2 * seq * pieces[0].shape[1] for pieces in streams),
            transcendentals=0,
        ),
        name=name,
    )(
        *[piece for pieces in streams for piece in pieces],
        *[part.array if isinstance(part, Columns) else part for part in ins],
    )


class Columns:
    def __init__(self, array, width, index):
        self.array = array
        self.index = index
        self.shape = (array.shape[0], width)


def resident(part):
    return pl.BlockSpec(
        part.shape, lambda i, *_: (0, part.index), pipeline_mode=pl.Buffered(1)
    )


def by_rows(rows, cols):
    return pl.BlockSpec((rows, cols), lambda i: (i, 0))


def project_qkv(tokens, weights, cos, sin):
    seq = sum(piece.shape[0] for piece in tokens)
    dim, cols = weights.shape
    width = cols // 3

    def body(x_ref, w_ref, cos_ref, sin_ref, out_ref):
        raw = dot(x_ref[...], w_ref[...])
        cos = wide_table(cos_ref[...], width)
        sin = wide_table(sin_ref[...], width)
        query = raw[:, :width]
        key = raw[:, width : 2 * width]
        query = (query * cos + partner_lanes(query, width) * sin) * (HEAD_DIM**-0.5)
        key = key * cos + partner_lanes(key, width) * sin
        out_ref[:, :width] = query.astype(BF16)
        out_ref[:, width : 2 * width] = key.astype(BF16)
        out_ref[:, 2 * width :] = raw[:, 2 * width :].astype(BF16)

    return streaming_call(
        [tokens],
        body,
        [weights, cos, sin],
        lambda rows: [resident(weights), by_rows(rows, cos.shape[1]), by_rows(rows, sin.shape[1])],
        jax.ShapeDtypeStruct((seq, cols), BF16),
        lambda rows: by_rows(rows, cols),
        "project_qkv",
        2 * seq * dim * cols,
        2 * (dim * cols + seq * cols),
    )


def pull_back_out(tokens, w_out):
    seq = sum(piece.shape[0] for piece in tokens)
    dim, width = w_out.shape

    def body(x_ref, w_ref, out_ref):
        out_ref[...] = dot(x_ref[...], w_ref[...]).astype(BF16)

    return streaming_call(
        [tokens],
        body,
        [w_out],
        lambda rows: [resident(w_out)],
        jax.ShapeDtypeStruct((seq, width), BF16),
        lambda rows: by_rows(rows, width),
        "pull_back_out",
        2 * seq * dim * width,
        2 * (dim * width + seq * width),
    )


def mlp_body(x_ref, gy_ref, gu_ref, down_ref, hid_ref, dgu_ref):
    cols = hid_ref.shape[1]
    both = dot(x_ref[...], gu_ref[...])
    d_hid = dot(gy_ref[...], down_ref[...])
    gp = both[:, :cols]
    up = both[:, cols:]
    sig = jax.nn.sigmoid(gp)
    silu = gp * sig
    hid_ref[...] = (silu * up).astype(BF16)
    dgu_ref[:, :cols] = (d_hid * up * sig * (1.0 + gp * (1.0 - sig))).astype(BF16)
    dgu_ref[:, cols:] = (d_hid * silu).astype(BF16)


def mlp_products(tokens, gy, w_gu, w_down):
    seq = sum(piece.shape[0] for piece in tokens)
    dim, cols = w_down.shape
    return streaming_call(
        [tokens, gy],
        mlp_body,
        [w_gu, w_down],
        lambda rows: [resident(w_gu), resident(w_down)],
        [jax.ShapeDtypeStruct((seq, cols), BF16), jax.ShapeDtypeStruct((seq, 2 * cols), BF16)],
        lambda rows: [by_rows(rows, cols), by_rows(rows, 2 * cols)],
        "mlp_products",
        6 * seq * dim * cols,
        2 * (3 * dim * cols + 3 * seq * cols),
    )


def partial_sums(lefts, rights, side, got=None):
    seq = lefts[0].shape[0]
    dim = rights[0].shape[0]
    rows = seq // 2
    count = len(lefts)
    wide = lax.axis_size("wide")
    chunk = seq // wide
    split = got is not None and bits_of(wide) == 3 and chunk % 32 == 0
    block = chunk if split else min(512, rows)
    steps = rows // block
    half = block // 2

    def kernel(*refs):
        total = None
        for left, right in zip(refs[:count], refs[count : 2 * count]):
            term = dot(left[...], right[...], NT)
            total = term if total is None else total + term
        if got is None:
            refs[-1][...] = total.astype(BF16)
            return
        total = total + refs[2 * count][...].astype(F32)
        if not split:
            refs[-1][...] = total.astype(BF16)
            return
        keep_low, keep_high, send_x, send_y = refs[-4:]
        step = pl.program_id(0)
        low = total[:half].astype(BF16)
        high = total[half:].astype(BF16)

        @pl.when(step % 2 == 0)
        def _():
            keep_low[...] = low

        @pl.when(step % 2 == 1)
        def _():
            send_x[...] = low

        @pl.when(step < 2)
        def _():
            keep_high[...] = high

        @pl.when(step >= 2)
        def _():
            send_y[...] = high

    in_specs = [
        pl.BlockSpec((block, left.shape[1]), lambda i: (side * steps + i, 0)) for left in lefts
    ] + [resident(right) for right in rights]
    ins = list(lefts) + [right.array for right in rights]
    if got is not None:
        in_specs.append(by_rows(block, dim))
        ins.append(got)
    if split:
        out_shape = [jax.ShapeDtypeStruct((2 * half, dim), BF16)] * 4
        out_specs = [
            pl.BlockSpec((half, dim), lambda i: (i // 2, 0)),
            pl.BlockSpec((half, dim), lambda i: (jnp.minimum(i, 1), 0)),
            pl.BlockSpec((half, dim), lambda i: (i // 2, 0)),
            pl.BlockSpec((half, dim), lambda i: (jnp.maximum(i - 2, 0), 0)),
        ]
    else:
        out_shape = jax.ShapeDtypeStruct((rows, dim), BF16)
        out_specs = by_rows(block, dim)
    depth = sum(left.shape[1] for left in lefts)
    return pl.pallas_call(
        kernel,
        out_shape=out_shape,
        grid=(steps,),
        in_specs=in_specs,
        out_specs=out_specs,
        compiler_params=params_for(),
        cost_estimate=cost(
            flops=2 * rows * depth * dim,
            bytes_accessed=2 * (rows * depth + depth * dim + 2 * rows * dim),
            transcendentals=0,
        ),
        name="partial_sums",
    )(*ins)


def whole_sums(lefts, rights, place):
    seq = lefts[0].shape[0]
    dim = rights[0].shape[0]
    chunks = place.shape[0]
    block = seq // chunks
    count = len(lefts)

    def kernel(place_ref, *refs):
        total = None
        for left, right in zip(refs[:count], refs[count : 2 * count]):
            term = dot(left[...], right[...], NT)
            total = term if total is None else total + term
        refs[-1][...] = total.astype(BF16)

    depth = sum(left.shape[1] for left in lefts)
    return pl.pallas_call(
        kernel,
        out_shape=jax.ShapeDtypeStruct((seq, dim), BF16),
        grid_spec=pltpu.PrefetchScalarGridSpec(
            num_scalar_prefetch=1,
            grid=(chunks,),
            in_specs=[
                pl.BlockSpec((block, left.shape[1]), lambda i, at: (at[i], 0)) for left in lefts
            ]
            + [resident(right) for right in rights],
            out_specs=pl.BlockSpec((block, dim), lambda i, at: (i, 0)),
        ),
        compiler_params=params_for(),
        cost_estimate=cost(
            flops=2 * seq * depth * dim,
            bytes_accessed=2 * (seq * depth + depth * dim + seq * dim),
            transcendentals=0,
        ),
        name="whole_sums",
    )(place, *lefts, *[right.array for right in rights])


def halves(array):
    if isinstance(array, (list, tuple)):
        return [(half, 0) for half in array]
    return [(array, 0), (array, 1)]


def weight_grad(lefts, rights, seq, before=None, parts=1):
    seq //= 2
    lefts = [pair for left in lefts for pair in halves(left)]
    rights = [pair for right in rights for pair in halves(right)]
    height = lefts[0][0].shape[1]
    cols = rights[0][0].shape[1]
    tall = min(512 if height < 1024 else 256, height)
    wide = min(1024, cols)
    count = len(lefts)
    first = 0 if before is None else (parts - 1) * height // tall

    def kernel(*refs):
        total = None
        for left, right in zip(refs[:count], refs[count : 2 * count]):
            term = dot(left[...], right[...], TN)
            total = term if total is None else total + term
        refs[-1][...] = total.astype(BF16)

    return pl.pallas_call(
        kernel,
        out_shape=jax.ShapeDtypeStruct((parts * height, cols), BF16),
        grid=(cols // wide, height // tall),
        in_specs=[pl.BlockSpec((seq, tall), lambda n, m, p=p: (p, m)) for _, p in lefts]
        + [pl.BlockSpec((seq, wide), lambda n, m, p=p: (p, n)) for _, p in rights]
        + [pl.BlockSpec(memory_space=pl.ANY)] * (before is not None),
        out_specs=pl.BlockSpec((tall, wide), lambda n, m: (m + first, n)),
        input_output_aliases={} if before is None else {2 * count: 0},
        compiler_params=params_for(),
        cost_estimate=cost(
            flops=2 * seq * height * cols * count,
            bytes_accessed=2 * count * (seq * height * (cols // wide) + seq * cols),
            transcendentals=0,
        ),
        name="weight_grad",
    )(
        *[a for a, _ in lefts],
        *[a for a, _ in rights],
        *([] if before is None else [before]),
    )


def head_stack(block, heads):
    lanes = lax.broadcasted_iota(jnp.int32, block.shape, 1) // HEAD_DIM
    zero = jnp.zeros_like(block)
    return jnp.concatenate([jnp.where(lanes == h, block, zero) for h in range(heads)], axis=0)


def block_mask(first_key, first_query, begins, size):
    keys = first_key + lax.broadcasted_iota(jnp.int32, (size, size), 0)
    queries = first_query + lax.broadcasted_iota(jnp.int32, (size, size), 1)
    return (keys <= queries) & (keys >= begins)


def forward_kernel(heads, blocks, size, low_ref, place_ref, begins_ref, qkv_ref, att_ref, lse_ref, vt_ref):
    width = heads * HEAD_DIM

    def spin(b, carry):
        rows = pl.ds(pl.multiple_of(place_ref[b] * size, size), size)
        vt_ref[b] = qkv_ref[rows, 2 * width :].astype(F32).T.astype(BF16)
        return carry

    lax.fori_loop(0, blocks, spin, 0)

    def one_query_block(i, carry):
        rows = pl.ds(pl.multiple_of(place_ref[i] * size, size), size)
        stack = head_stack(qkv_ref[rows, :width], heads)
        begins = begins_ref[i]

        def one_key_block(j, state):
            maxes, totals, sums = state
            keys = pl.ds(pl.multiple_of(place_ref[j] * size, size), size)
            scores = dot(qkv_ref[keys, width : 2 * width], stack, NT)
            allowed = block_mask(j * size, i * size, begins, size)
            new_maxes, new_totals, new_sums = [], [], []
            for h in range(heads):
                part = jnp.where(allowed, scores[:, h * size : (h + 1) * size], NEG)
                peak = jnp.maximum(maxes[h], jnp.max(part, axis=0, keepdims=True))
                fade = jnp.exp(maxes[h] - peak)
                probs = jnp.exp(part - peak)
                new_maxes.append(peak)
                new_totals.append(totals[h] * fade + jnp.sum(probs, axis=0, keepdims=True))
                values_t = vt_ref[j, h * HEAD_DIM : (h + 1) * HEAD_DIM, :]
                new_sums.append(sums[h] * fade + dot(values_t, probs.astype(BF16)))
            return (tuple(new_maxes), tuple(new_totals), tuple(new_sums))

        start = (
            tuple(jnp.full((1, size), NEG, F32) for _ in range(heads)),
            tuple(jnp.zeros((1, size), F32) for _ in range(heads)),
            tuple(jnp.zeros((HEAD_DIM, size), F32) for _ in range(heads)),
        )
        maxes, totals, sums = lax.fori_loop(low_ref[i], i + 1, one_key_block, start)
        outs = jnp.concatenate([sums[h] / totals[h] for h in range(heads)], axis=0)
        att_ref[rows, :] = outs.T.astype(BF16)
        for h in range(heads):
            lse_ref[i, h : h + 1, :] = maxes[h] + jnp.log(totals[h])
        return carry

    lax.fori_loop(0, blocks, one_query_block, 0)


def attend_forward(qkv, low, place, begins, heads):
    seq = qkv.shape[0]
    blocks, _, size = begins.shape
    width = heads * HEAD_DIM
    pairs = seq * seq // 3
    return pl.pallas_call(
        functools.partial(forward_kernel, heads, blocks, size),
        out_shape=(
            jax.ShapeDtypeStruct((seq, width), BF16),
            jax.ShapeDtypeStruct((blocks, heads, size), F32),
        ),
        in_specs=[smem(), smem(), vmem(), vmem()],
        out_specs=(vmem(), vmem()),
        scratch_shapes=[pltpu.VMEM((blocks, width, size), BF16)],
        compiler_params=params_for(),
        cost_estimate=cost(
            flops=16 * pairs * width,
            bytes_accessed=2 * seq * width * 4,
            transcendentals=pairs * heads,
        ),
        name="attend_forward",
    )(low, place, begins, qkv)


def backward_kernel(
    heads,
    blocks,
    size,
    low_ref,
    place_ref,
    begins_ref,
    qkv_ref,
    att_ref,
    grad_ref,
    lse_ref,
    cos_ref,
    sin_ref,
    out_ref,
    kt_ref,
    dk_ref,
    dv_ref,
):
    width = heads * HEAD_DIM
    scale = HEAD_DIM**-0.5

    def spin(b, carry):
        rows = pl.ds(pl.multiple_of(place_ref[b] * size, size), size)
        kt_ref[b] = qkv_ref[rows, width : 2 * width].astype(F32).T.astype(BF16)
        dk_ref[b] = jnp.zeros((size, width), F32)
        dv_ref[b] = jnp.zeros((size, width), F32)
        return carry

    lax.fori_loop(0, blocks, spin, 0)

    def unrotate(values, rows):
        cos = wide_table(cos_ref[rows, :], width)
        sin = wide_table(sin_ref[rows, :], width)
        return values * cos - partner_lanes(values, width) * sin

    def one_query_block(i, carry):
        rows = pl.ds(pl.multiple_of(place_ref[i] * size, size), size)
        q_stack = head_stack(qkv_ref[rows, :width], heads)
        grad = grad_ref[rows, :]
        g_stack = head_stack(grad, heads)
        product = (grad.astype(F32) * att_ref[rows, :].astype(F32)).T
        deltas = [
            jnp.sum(product[h * HEAD_DIM : (h + 1) * HEAD_DIM], axis=0, keepdims=True)
            for h in range(heads)
        ]
        begins = begins_ref[i]

        def one_key_block(j, sums):
            keys = pl.ds(pl.multiple_of(place_ref[j] * size, size), size)
            scores = dot(qkv_ref[keys, width : 2 * width], q_stack, NT)
            grads = dot(qkv_ref[keys, 2 * width :], g_stack, NT)
            allowed = block_mask(j * size, i * size, begins, size)
            all_probs, all_ds, new_sums = [], [], []
            for h in range(heads):
                span = slice(h * size, (h + 1) * size)
                part = jnp.where(allowed, scores[:, span] - lse_ref[i, h : h + 1, :], NEG)
                probs = jnp.exp(part)
                d_scores = (probs * (grads[:, span] - deltas[h])).astype(BF16)
                all_probs.append(probs.astype(BF16))
                all_ds.append(d_scores)
                keys_t = kt_ref[j, h * HEAD_DIM : (h + 1) * HEAD_DIM, :]
                new_sums.append(sums[h] + dot(keys_t, d_scores))
            dv_ref[j] += dot(jnp.concatenate(all_probs, axis=1), g_stack)
            dk_ref[j] += dot(jnp.concatenate(all_ds, axis=1), q_stack)
            return tuple(new_sums)

        start = tuple(jnp.zeros((HEAD_DIM, size), F32) for _ in range(heads))
        sums = lax.fori_loop(low_ref[i], i + 1, one_key_block, start)
        query_grad = jnp.concatenate(sums, axis=0).T * scale
        out_ref[rows, :width] = unrotate(query_grad, rows).astype(BF16)
        return carry

    lax.fori_loop(0, blocks, one_query_block, 0)

    def finish(b, carry):
        rows = pl.ds(pl.multiple_of(place_ref[b] * size, size), size)
        out_ref[rows, width : 2 * width] = unrotate(dk_ref[b], rows).astype(BF16)
        out_ref[rows, 2 * width :] = dv_ref[b].astype(BF16)
        return carry

    lax.fori_loop(0, blocks, finish, 0)


def attend_backward(qkv, att, grad, lse, low, place, begins, cos, sin, heads):
    seq = qkv.shape[0]
    blocks, _, size = begins.shape
    width = heads * HEAD_DIM
    pairs = seq * seq // 3
    return pl.pallas_call(
        functools.partial(backward_kernel, heads, blocks, size),
        out_shape=jax.ShapeDtypeStruct((seq, 3 * width), BF16),
        in_specs=[smem(), smem()] + [vmem()] * 7,
        out_specs=vmem(),
        scratch_shapes=[
            pltpu.VMEM((blocks, width, size), BF16),
            pltpu.VMEM((blocks, size, width), F32),
            pltpu.VMEM((blocks, size, width), F32),
        ],
        compiler_params=params_for(),
        cost_estimate=cost(
            flops=40 * pairs * width,
            bytes_accessed=2 * seq * width * 10,
            transcendentals=pairs * heads,
        ),
        name="attend_backward",
    )(low, place, begins, qkv, att, grad, lse, cos, sin)


def row_facts(lengths, seq):
    wide = lax.axis_size("wide")
    me = lax.axis_index("wide")
    chunk = seq // wide
    docs = lengths.shape[0]
    upto = jnp.arange(docs)[:, None] <= jnp.arange(docs)[None, :]
    ends = jnp.sum(jnp.where(upto, lengths[:, None], 0), axis=0).astype(jnp.int32)

    def starts_of(tokens):
        before = jnp.where(ends[None, :] <= tokens[:, None], ends[None, :], jnp.int32(0))
        return jnp.max(before, axis=1)

    tokens = jnp.arange(seq, dtype=jnp.int32)
    begins = starts_of(tokens).reshape(wide, 1, chunk)
    low = begins[:, 0, 0] // chunk
    index = jnp.arange(wide, dtype=jnp.int32)
    place = place_of(index ^ me, wide)
    owner = me ^ offset_at(index, wide)
    here = (owner[:, None] * chunk + jnp.arange(chunk, dtype=jnp.int32)[None, :]).reshape(seq)
    position = (here - starts_of(here)).astype(F32)
    half_dim = HEAD_DIM // 2
    inverse = ROPE_BASE ** (-(jnp.arange(half_dim, dtype=F32) * 2.0) / HEAD_DIM)
    angles = position[:, None] * inverse[None, :]
    cos = jnp.cos(angles)
    sin = jnp.sin(angles)
    cos = jnp.concatenate([cos, cos, cos, cos], axis=1)
    sin = jnp.concatenate([-sin, sin, -sin, sin], axis=1)
    return low, place, begins, cos, sin


def norm_scale(values):
    return lax.rsqrt(jnp.mean(values * values, axis=-1, keepdims=True) + EPS)


def per_device(
    hidden_in,
    out_grad,
    doc_lengths,
    attn_gain,
    w_query,
    w_key,
    w_value,
    w_out,
    mlp_gain,
    w_gate,
    w_up,
    w_down,
):
    narrow = lax.axis_size("narrow")
    wide = lax.axis_size("wide")
    here = lax.axis_index("narrow")
    rows_here, chunk, dim = hidden_in.shape
    seq = chunk * wide
    width = w_query.shape[1]
    heads = width // HEAD_DIM

    def fetch(weight, axis):
        return lax.all_gather(weight, "narrow", axis=axis, tiled=True)

    gains = jnp.stack([attn_gain, mlp_gain])
    turned = [gains]
    for step in range(1, narrow):
        turned.append(
            lax.ppermute(gains, "narrow", [((i + step) % narrow, i) for i in range(narrow)])
        )
    order = (jnp.arange(narrow) - here) % narrow
    gains = jnp.take(jnp.stack(turned), order, axis=0)
    gains = jnp.swapaxes(gains, 0, 1).reshape(2, dim).astype(F32)
    attn_scale = gains[0]
    mlp_scale = gains[1]

    slots = Slots()
    gate, ends, turn = slots.gate, slots.ends, slots.turn
    hidden = w_gate.shape[1]
    cut = hidden // 2
    spans = [slice(0, cut), slice(cut, hidden)]
    first_own = jnp.concatenate([w_query, w_key, w_value, w_out.T], axis=1)
    first_set = fetch(first_own, 0)
    w_qkv = Columns(first_set, 3 * width, 0)
    full_out = Columns(first_set, width, 3)
    ffn_sets, full_gu, full_down = [], [], []

    def lay_out():
        for span in spans:
            own = [gate(w_gate)[:, span], gate(w_up)[:, span], gate(w_down)[span].T]
            own = ends(jnp.concatenate(own, axis=1))
            ffn_sets.append(fetch(own, 0))
            full_gu.append(Columns(ffn_sets[-1], 2 * cut, 0))
            full_down.append(Columns(ffn_sets[-1], cut, 2))


    rows = range(rows_here)
    last = rows_here - 1
    facts = {}
    residual = [hidden_in[r].astype(F32) for r in rows]
    inv_first = [norm_scale(residual[r]) for r in rows]
    normed = [residual[r] * inv_first[r] for r in rows]
    scaled_in = [(normed[r] * attn_scale).astype(BF16) for r in rows]

    attn_in, gy, mlp_in, branch = {}, {}, {}, {}
    qkv, att, lse, middle, inv_second = ({} for _ in range(5))
    grad_middle, gain_mlp, gain_attn, outputs, in_grads, d_qkv = ({} for _ in range(6))
    hid = {r: [] for r in rows}
    d_gu = {r: [] for r in rows}

    def know(r):
        facts[r] = row_facts(gate(doc_lengths[r]), seq)
        ends(facts[r][3])
        ends(facts[r][4])

    def first_of(halves):
        return [gate(halves[0])] + list(halves[1:])

    def project(r):
        _, _, _, cos, sin = facts[r]
        qkv[r] = ends(project_qkv(first_of(attn_in[r].halves), w_qkv, cos, sin))

    def attend(r):
        low, place, begins, _, _ = facts[r]
        att[r], lse[r] = attend_forward(gate(qkv[r]), low, place, begins, heads)
        ends(att[r])

    def spread(lefts, rights):
        return Scatter(slots, lefts, rights)

    def after_attention(r, total):
        middle[r] = gate(hidden_in[r]).astype(F32) + total
        inv_second[r] = norm_scale(middle[r])
        mlp_in[r] = Gather(slots, (middle[r] * inv_second[r] * mlp_scale).astype(BF16))

    def mlp(r, part):
        one, two = mlp_products(
            first_of(mlp_in[r].halves), gy[r].halves, full_gu[part], full_down[part]
        )
        ends(one)
        hid[r].append(one)
        d_gu[r].append(two)

    def after_mlp(r, total):
        total = gate(total).astype(F32)
        normed_mid = gate(middle[r]) * inv_second[r]
        gain_mlp[r] = jnp.sum(total * normed_mid, axis=0)
        scaled = total * mlp_scale
        grad_middle[r] = out_grad[r].astype(F32) + inv_second[r] * (
            scaled - normed_mid * jnp.mean(scaled * normed_mid, axis=-1, keepdims=True)
        )
        branch[r] = Gather(slots, grad_middle[r].astype(BF16))

    def back_attention(r):
        low, place, begins, cos, sin = facts[r]
        grad_att = pull_back_out(first_of(branch[r].halves), full_out)
        d_qkv[r] = ends(
            attend_backward(
                qkv[r], att[r], grad_att, lse[r], low, place, begins, cos, sin, heads
            )
        )

    def after_back(r, total):
        normed_in = gate(hidden_in[r]).astype(F32) * inv_first[r]
        gain_attn[r] = jnp.sum(total * normed_in, axis=0)
        scaled = total * attn_scale
        in_grads[r] = (
            grad_middle[r]
            + inv_first[r]
            * (scaled - normed_in * jnp.mean(scaled * normed_in, axis=-1, keepdims=True))
        ).astype(BF16)

    def grad_factors(lefts, rights):
        lefts = [lefts[r] for r in rows]
        lefts[0] = first_of(lefts[0]) if isinstance(lefts[0], list) else gate(lefts[0])
        return lefts, [rights[r] for r in rows]

    def grad_of(lefts, rights, table, key, wait=True, axis=0):
        grad = ends(weight_grad(*grad_factors(lefts, rights), seq))

        def start():
            table[key] = lax.psum_scatter(
                gate(grad) if wait else grad, "narrow", scatter_dimension=axis, tiled=True
            )

        if wait:
            slots.later(start)
        else:
            start()

    def both(table):
        return [table[r] for r in rows]

    def halves_of(table):
        return {r: table[r].halves for r in rows}

    def part_of(table, part):
        return {r: table[r][part] for r in rows}

    sums, down, grad_gu, grad_down, grad_attn = {}, {}, [None, None], [None, None], {}

    def out_sum(r):
        sums[r] = spread([att[r]], [full_out])

    def mlp_sum(r):
        whole = ends(whole_sums(first_of(d_gu[r]), full_gu, facts[r][1]))

        def start():
            sums[r] = lax.psum_scatter(gate(whole), "wide", scatter_dimension=0, tiled=True)

        slots.later(start)

    def back_sum(r):
        sums[r] = spread([d_qkv[r]], [w_qkv])

    def down_sum(r):
        down[r] = spread(hid[r], full_down)

    def gu_grad(part):
        grad_of(halves_of(mlp_in), part_of(d_gu, part), grad_gu, part)

    def down_grad(part):
        factors = grad_factors(part_of(hid, part), halves_of(gy))
        if part == 0:
            grad_down[0] = ends(weight_grad(*factors, seq, None, 2))
            return
        grad = ends(weight_grad(*factors, seq, grad_down[0], 2))

        def start():
            grad_down[0] = lax.psum_scatter(
                gate(grad), "narrow", scatter_dimension=1, tiled=True
            )

        slots.later(start)

    one, two = 0, last
    attn_in[one] = Gather(slots, scaled_in[one])
    ends(first_own)
    turn()
    attn_in[one].far()
    know(one)
    lay_out()
    turn()
    attn_in[one].core()
    attn_in[two] = Gather(slots, scaled_in[two])
    know(two)
    ends(first_set)
    turn()
    project(one)
    attn_in[two].far()
    turn()
    attend(one)
    attn_in[two].core()
    gy[one] = Gather(slots, out_grad[one])
    turn()
    out_sum(one)
    sums[one].core()
    project(two)
    gy[one].far()
    turn()
    sums[one].even()
    gy[one].core()
    gy[two] = Gather(slots, out_grad[two])
    turn()
    attend(two)
    sums[one].near()
    ends(ffn_sets[0])
    turn()
    out_sum(two)
    sums[one].last()
    gy[two].far()
    turn()
    after_attention(one, sums[one].total)
    sums[two].core()
    gy[two].core()
    turn()
    sums[two].even()
    mlp_in[one].far()
    turn()
    mlp_in[one].core()
    sums[two].near()
    ends(ffn_sets[1])
    turn()
    mlp(one, 0)
    sums[two].last()
    turn()
    mlp(one, 1)
    after_attention(two, sums[two].total)
    turn()
    mlp_sum(one)
    mlp_in[two].far()
    turn()
    down_sum(one)
    mlp_in[two].core()
    turn()
    mlp(two, 0)
    down[one].core()
    turn()
    mlp(two, 1)
    turn()
    mlp_sum(two)
    ends(sums[one])
    turn()
    gu_grad(0)
    after_mlp(one, sums[one])
    turn()
    gu_grad(1)
    branch[one].far()
    turn()
    down_sum(two)
    down[one].even()
    branch[one].core()
    turn()
    back_attention(one)
    down[one].near()
    down[two].core()
    ends(sums[two])
    turn()
    back_sum(one)
    down[two].even()
    after_mlp(two, sums[two])
    turn()
    down_grad(0)
    sums[one].core()
    branch[two].far()
    down[one].last()
    turn()
    sums[one].even()
    down_grad(1)
    branch[two].core()
    down[two].near()
    ends(grad_gu[0])
    turn()
    grad_of(att, halves_of(branch), grad_attn, "out", axis=1)
    back_attention(two)
    sums[one].near()
    down[two].last()
    turn()
    back_sum(two)
    sums[one].last()
    ends(grad_gu[1])
    turn()
    sums[two].core()
    turn()
    sums[two].even()
    ends(grad_down[0])
    turn()
    grad_of(halves_of(attn_in), d_qkv, grad_attn, "qkv", False)
    sums[two].near()
    turn()
    sums[two].last()
    turn()
    for r in rows:
        outputs[r] = (middle[r] + down[r].total).astype(BF16)
        after_back(r, sums[r].total)

    gains = jnp.stack([sum(both(part)[1:], part[one]) for part in (gain_attn, gain_mlp)])
    for axis in ("narrow", "wide"):
        count = lax.axis_size(axis)
        me = lax.axis_index(axis)
        for bit in reversed(range(bits_of(count))):
            size = gains.shape[1] // 2
            mine = (me >> bit) & 1
            sent = lax.dynamic_slice_in_dim(gains, (1 - mine) * size, size, 1)
            kept = lax.dynamic_slice_in_dim(gains, mine * size, size, 1)
            gains = kept + lax.ppermute(sent, axis, [(i, i ^ (1 << bit)) for i in range(count)])

    grad_gu = [grad.astype(F32) for grad in grad_gu]
    grad_attn = {key: grad.astype(F32) for key, grad in grad_attn.items()}
    grad_gate = [piece[:, :cut] for piece in grad_gu]
    grad_up = [piece[:, cut:] for piece in grad_gu]
    return (
        jnp.stack(both(outputs)),
        jnp.stack(both(in_grads)),
        gains[0],
        grad_attn["qkv"][:, :width],
        grad_attn["qkv"][:, width : 2 * width],
        grad_attn["qkv"][:, 2 * width :],
        grad_attn["out"],
        gains[1],
        jnp.concatenate(grad_gate, axis=1),
        jnp.concatenate(grad_up, axis=1),
        grad_down[0].astype(F32),
    )


def solution(mesh):
    in_specs = (
        P("narrow", "wide", None),
        P("narrow", "wide", None),
        P("narrow", None),
        P("narrow"),
        P("narrow", "wide"),
        P("narrow", "wide"),
        P("narrow", "wide"),
        P("wide", "narrow"),
        P("narrow"),
        P("narrow", "wide"),
        P("narrow", "wide"),
        P("wide", "narrow"),
    )
    out_specs = (
        P("narrow", "wide", None),
        P("narrow", "wide", None),
        P(("narrow", "wide")),
        P("narrow", "wide"),
        P("narrow", "wide"),
        P("narrow", "wide"),
        P("wide", "narrow"),
        P(("narrow", "wide")),
        P("narrow", "wide"),
        P("narrow", "wide"),
        P("wide", "narrow"),
    )
    return jax.shard_map(
        per_device, mesh=mesh, in_specs=in_specs, out_specs=out_specs, check_vma=False
    )
```

```python
import functools

import jax
import jax.numpy as jnp
from jax import lax
from jax.experimental import pallas as pl
from jax.experimental.pallas import tpu as pltpu
from jax.sharding import PartitionSpec as P

HEAD_DIM = 64
EPS = 1e-05
NEG = -1e30
ROPE_BASE = 130000.0
F32 = jnp.float32
BF16 = jnp.bfloat16
NN = (((1,), (0,)), ((), ()))
NT = (((1,), (1,)), ((), ()))
TN = (((0,), (0,)), ((), ()))
VMEM_LIMIT = 60 * 1024 * 1024
COST = 0.02


def dot(left, right, dims=NN):
    return lax.dot_general(left, right, dims, preferred_element_type=F32)


def params_for(**extra):
    return pltpu.CompilerParams(vmem_limit_bytes=VMEM_LIMIT, **extra)


def cost(flops, bytes_accessed, transcendentals):
    return pl.CostEstimate(
        flops=int(flops * COST),
        bytes_accessed=int(bytes_accessed * COST),
        transcendentals=int(transcendentals * COST),
    )


def vmem():
    return pl.BlockSpec(memory_space=pltpu.VMEM)


def smem():
    return pl.BlockSpec(memory_space=pltpu.SMEM)


def bits_of(count):
    return count.bit_length() - 1


def offset_at(place, count):
    top = bits_of(count) - 1
    return ((place << 1) & (count - 1)) | (place >> top)


def place_of(offset, count):
    top = bits_of(count) - 1
    return (offset >> 1) | ((offset & 1) << top)


def swap(block, bit):
    count = lax.axis_size("wide")
    return lax.ppermute(block, "wide", [(i, i ^ (1 << bit)) for i in range(count)])


def after(value, *others):
    return lax.optimization_barrier((value,) + others)[0] if others else value


class Slots:
    def __init__(self):
        self.now = []
        self.then = []
        self.waiting = []

    def later(self, action):
        self.waiting.append(action)

    def gate(self, value):
        if isinstance(value, Columns):
            return Columns(after(value.array, *self.now), value.shape[1], value.index)
        return after(value, *self.now)

    def ends(self, value):
        self.then.append(value)
        return value

    def turn(self):
        self.now = self.then or self.now
        self.then = []
        waiting, self.waiting = self.waiting, []
        for action in waiting:
            action()

    def swap(self, block, bit, axis="wide", hold=True):
        count = lax.axis_size(axis)
        pairs = [(i, i ^ (1 << bit)) for i in range(count)]
        got = lax.ppermute(self.gate(block), axis, pairs)
        return self.ends(got) if hold else got


class Gather:
    def __init__(self, slots, block):
        self.slots = slots
        self.block = block
        chip_bits = bits_of(lax.axis_size("wide")) - 1
        self.plain = not (chip_bits == 2 and block.shape[0] % 32 == 0)
        if not self.plain:
            self.from_x = slots.swap(block, 1)
            self.from_y = slots.swap(block, 2)

    def far(self):
        if not self.plain:
            half = self.block.shape[0] // 2
            self.far_low = self.slots.swap(self.from_y[:half], 1)
            self.far_high = self.slots.swap(self.from_x[half:], 2)

    def core(self):
        if self.plain:
            pieces = [self.block]
            for bit in range(1, bits_of(lax.axis_size("wide"))):
                pieces = pieces + [self.slots.swap(piece, bit) for piece in pieces]
        else:
            pieces = [self.block, self.from_x, self.from_y, self.far_low, self.far_high]
        own = jnp.concatenate(pieces, axis=0)
        self.halves = [own, self.slots.swap(own, 0)]


class Offloaded:
    def __init__(self, slots, block):
        self.slots = slots
        count = lax.axis_size("wide")
        groups = [list(range(core, count, 2)) for core in range(2)]
        self.chips = lax.all_gather(
            slots.gate(block), "wide", axis_index_groups=groups, axis=0, tiled=True
        )

    def core(self):
        chips = lax.axis_size("wide") // 2
        rows = self.chips.shape[0] // chips
        here = lax.axis_index("wide") // 2
        own = jnp.concatenate(
            [
                lax.dynamic_slice_in_dim(self.chips, (here ^ chip) * rows, rows)
                for chip in range(chips)
            ],
            axis=0,
        )
        self.halves = [own, self.slots.swap(own, 0)]


class Scatter:
    def __init__(self, slots, lefts, rights):
        self.slots = slots
        self.factors = (lefts, rights)
        self.sent = self.product(1)

    def product(self, side, got=None):
        lefts, rights = self.factors
        lefts = [self.slots.gate(lefts[0])] + list(lefts[1:])
        made = partial_sums(lefts, rights, side, got)
        self.slots.ends(made[0] if isinstance(made, (list, tuple)) else made)
        return made

    def core(self):
        self.got = self.slots.swap(self.sent, 0)

    def even(self):
        self.kept = self.product(0, self.got)

    def near(self):
        if isinstance(self.kept, (tuple, list)):
            self.got_x = self.slots.swap(self.kept[2], 1)
            self.got_y = self.slots.swap(self.kept[3], 2)
            return
        kept = self.kept
        for bit in reversed(range(bits_of(lax.axis_size("wide")) - 1)):
            rows = kept.shape[0] // 2
            got = self.slots.swap(kept[rows:], bit + 1)
            kept = (kept[:rows].astype(F32) + got.astype(F32)).astype(BF16)
        self.total = kept.astype(F32)

    def last(self, hold=True):
        if not isinstance(self.kept, (tuple, list)):
            return
        keep_low, keep_high = self.kept[:2]
        half = keep_low.shape[0] // 2
        far_low = (keep_low[half:].astype(F32) + self.got_x[half:].astype(F32)).astype(BF16)
        far_high = (keep_high[half:].astype(F32) + self.got_y[half:].astype(F32)).astype(BF16)
        low = self.slots.swap(far_low, 2, hold=hold)
        high = self.slots.swap(far_high, 1, hold=hold)
        low = keep_low[:half].astype(F32) + self.got_x[:half].astype(F32) + low.astype(F32)
        high = keep_high[:half].astype(F32) + self.got_y[:half].astype(F32) + high.astype(F32)
        self.total = jnp.concatenate([low, high], axis=0)


def partner_lanes(values, width):
    lanes = lax.broadcasted_iota(jnp.int32, values.shape, 1)
    first = (lanes % HEAD_DIM) < HEAD_DIM // 2
    half = HEAD_DIM // 2
    return jnp.where(first, pltpu.roll(values, width - half, 1), pltpu.roll(values, half, 1))


def wide_table(table, width):
    copies = width // table.shape[1]
    return jnp.concatenate([table] * copies, axis=1) if copies > 1 else table


def streaming_call(streams, body, ins, in_specs, outs, out_specs, name, flops, moved):
    seq = sum(piece.shape[0] for piece in streams[0])
    rows = min(512, streams[0][0].shape[0])
    steps = seq // rows
    plan = []
    for number, pieces in enumerate(streams):
        first = 0
        for piece in pieces:
            plan.append((number, first, piece.shape[0]))
            first += piece.shape[0]
    count, groups = len(plan), len(streams)

    def kernel(*refs):
        piece_refs, rest = refs[:count], refs[count:]
        middle_refs, buffers, sems = rest[: -groups - 1], rest[-groups - 1 : -1], rest[-1]
        step = pl.program_id(0)

        def copies(block, slot):
            found = []
            for ref, (number, first, size) in zip(piece_refs, plan):
                place = block * rows - first
                if 0 <= place < size:
                    source = ref.at[pl.ds(place, rows)]
                    found.append(
                        pltpu.make_async_copy(
                            source, buffers[number].at[slot], sems.at[number, slot]
                        )
                    )
            return found

        for block in range(steps):

            @pl.when(step == (0 if block == 0 else block - 1))
            def _():
                for copy in copies(block, block % 2):
                    copy.start()

        for block in range(steps):

            @pl.when(step == block)
            def _():
                for copy in copies(block, block % 2):
                    copy.wait()

        slot = lax.rem(step, 2)
        body(*[buffer.at[slot] for buffer in buffers], *middle_refs)

    return pl.pallas_call(
        kernel,
        out_shape=outs,
        grid=(steps,),
        in_specs=[pl.BlockSpec(memory_space=pl.ANY)] * count + in_specs(rows),
        out_specs=out_specs(rows),
        scratch_shapes=[pltpu.VMEM((2, rows, pieces[0].shape[1]), BF16) for pieces in streams]
        + [pltpu.SemaphoreType.DMA((groups, 2))],
        compiler_params=params_for(),
        cost_estimate=cost(
            flops=flops,
            bytes_accessed=moved + sum(2 * seq * pieces[0].shape[1] for pieces in streams),
            transcendentals=0,
        ),
        name=name,
    )(
        *[piece for pieces in streams for piece in pieces],
        *[part.array if isinstance(part, Columns) else part for part in ins],
    )


class Columns:
    def __init__(self, array, width, index):
        self.array = array
        self.index = index
        self.shape = (array.shape[0], width)


def columns_of(array):
    return array if isinstance(array, Columns) else Columns(array, array.shape[1], 0)


def resident(part):
    return pl.BlockSpec(
        part.shape, lambda i, *_: (0, part.index), pipeline_mode=pl.Buffered(1)
    )


def by_rows(rows, cols):
    return pl.BlockSpec((rows, cols), lambda i: (i, 0))


def project_qkv(tokens, weights, cos, sin):
    seq = sum(piece.shape[0] for piece in tokens)
    dim, cols = weights.shape
    width = cols // 3

    def body(x_ref, w_ref, cos_ref, sin_ref, out_ref):
        raw = dot(x_ref[...], w_ref[...])
        cos = wide_table(cos_ref[...], width)
        sin = wide_table(sin_ref[...], width)
        query = raw[:, :width]
        key = raw[:, width : 2 * width]
        query = (query * cos + partner_lanes(query, width) * sin) * (HEAD_DIM**-0.5)
        key = key * cos + partner_lanes(key, width) * sin
        out_ref[:, :width] = query.astype(BF16)
        out_ref[:, width : 2 * width] = key.astype(BF16)
        out_ref[:, 2 * width :] = raw[:, 2 * width :].astype(BF16)

    return streaming_call(
        [tokens],
        body,
        [weights, cos, sin],
        lambda rows: [resident(weights), by_rows(rows, cos.shape[1]), by_rows(rows, sin.shape[1])],
        jax.ShapeDtypeStruct((seq, cols), BF16),
        lambda rows: by_rows(rows, cols),
        "project_qkv",
        2 * seq * dim * cols,
        2 * (dim * cols + seq * cols),
    )


def pull_back_out(tokens, w_out):
    seq = sum(piece.shape[0] for piece in tokens)
    dim, width = w_out.shape

    def body(x_ref, w_ref, out_ref):
        out_ref[...] = dot(x_ref[...], w_ref[...]).astype(BF16)

    return streaming_call(
        [tokens],
        body,
        [w_out],
        lambda rows: [resident(w_out)],
        jax.ShapeDtypeStruct((seq, width), BF16),
        lambda rows: by_rows(rows, width),
        "pull_back_out",
        2 * seq * dim * width,
        2 * (dim * width + seq * width),
    )


def mlp_products(tokens, gy, sets):
    seq = sum(piece.shape[0] for piece in tokens)
    dim = tokens[0].shape[1]
    cut = sets[0].shape[1] // 3
    parts = len(sets)
    rows = min(512, tokens[0].shape[0])
    steps = seq // rows
    streams = [tokens, gy]
    count = sum(len(pieces) for pieces in streams)

    def kernel(*refs):
        piece_refs, set_refs, rest = refs[:count], refs[count : count + parts], refs[count + parts :]
        hid_ref, dgu_ref, x_buffer, gy_buffer, set_buffer, sems, set_sems = rest
        step = pl.program_id(0)

        def copies(number):
            found, at = [], 0
            slot = number % 2
            for stream, (pieces, buffer) in enumerate(zip(streams, (x_buffer, gy_buffer))):
                first = 0
                for piece in pieces:
                    place = (number % steps) * rows - first
                    if 0 <= place < piece.shape[0]:
                        source = piece_refs[at].at[pl.ds(place, rows)]
                        found.append(
                            pltpu.make_async_copy(source, buffer.at[slot], sems.at[stream, slot])
                        )
                    first += piece.shape[0]
                    at += 1
            return found

        loads = [
            pltpu.make_async_copy(set_refs[p], set_buffer.at[p], set_sems.at[p])
            for p in range(parts)
        ]

        @pl.when(step == 0)
        def _():
            for copy in copies(0) + loads:
                copy.start()

        for number in range(parts * steps):

            @pl.when(step == number)
            def _():
                if number + 1 < parts * steps:
                    for copy in copies(number + 1):
                        copy.start()
                for copy in copies(number):
                    copy.wait()
                if number % steps == 0:
                    loads[number // steps].wait()

        slot = lax.rem(step, 2)
        weights = set_buffer.at[step // steps]
        both = dot(x_buffer[slot], weights[:, : 2 * cut])
        d_hid = dot(gy_buffer[slot], weights[:, 2 * cut :])
        gp = both[:, :cut]
        up = both[:, cut:]
        sig = jax.nn.sigmoid(gp)
        silu = gp * sig
        hid_ref[...] = (silu * up).astype(BF16)
        dgu_ref[:, :cut] = (d_hid * up * sig * (1.0 + gp * (1.0 - sig))).astype(BF16)
        dgu_ref[:, cut:] = (d_hid * silu).astype(BF16)

    def out_map(s):
        return (s % steps, s // steps)

    return pl.pallas_call(
        kernel,
        out_shape=[
            jax.ShapeDtypeStruct((seq, parts * cut), BF16),
            jax.ShapeDtypeStruct((seq, 2 * parts * cut), BF16),
        ],
        grid=(parts * steps,),
        in_specs=[pl.BlockSpec(memory_space=pl.ANY)] * (count + parts),
        out_specs=[pl.BlockSpec((rows, cut), out_map), pl.BlockSpec((rows, 2 * cut), out_map)],
        scratch_shapes=[
            pltpu.VMEM((2, rows, dim), BF16),
            pltpu.VMEM((2, rows, dim), BF16),
            pltpu.VMEM((parts, dim, 3 * cut), BF16),
            pltpu.SemaphoreType.DMA((2, 2)),
            pltpu.SemaphoreType.DMA((parts,)),
        ],
        compiler_params=params_for(),
        cost_estimate=cost(
            flops=6 * seq * dim * cut * parts,
            bytes_accessed=2 * parts * (2 * seq * dim + 3 * dim * cut + 3 * seq * cut),
            transcendentals=seq * cut * parts,
        ),
        name="mlp_products",
    )(*[piece for pieces in streams for piece in pieces], *sets)


def partial_sums(lefts, rights, side, got=None):
    lefts = [columns_of(left) for left in lefts]
    seq = lefts[0].shape[0]
    dim = rights[0].shape[0]
    rows = seq // 2
    count = len(lefts)
    wide = lax.axis_size("wide")
    chunk = seq // wide
    split = got is not None and bits_of(wide) == 3 and chunk % 32 == 0
    block = chunk if split else min(512, rows)
    steps = rows // block
    half = block // 2

    def kernel(*refs):
        total = None
        for left, right in zip(refs[:count], refs[count : 2 * count]):
            term = dot(left[...], right[...], NT)
            total = term if total is None else total + term
        if got is None:
            refs[-1][...] = total.astype(BF16)
            return
        total = total + refs[2 * count][...].astype(F32)
        if not split:
            refs[-1][...] = total.astype(BF16)
            return
        keep_low, keep_high, send_x, send_y = refs[-4:]
        step = pl.program_id(0)
        low = total[:half].astype(BF16)
        high = total[half:].astype(BF16)

        @pl.when(step % 2 == 0)
        def _():
            keep_low[...] = low

        @pl.when(step % 2 == 1)
        def _():
            send_x[...] = low

        @pl.when(step < 2)
        def _():
            keep_high[...] = high

        @pl.when(step >= 2)
        def _():
            send_y[...] = high

    in_specs = [
        pl.BlockSpec((block, left.shape[1]), lambda i, left=left: (side * steps + i, left.index))
        for left in lefts
    ] + [resident(right) for right in rights]
    ins = [left.array for left in lefts] + [right.array for right in rights]
    if got is not None:
        in_specs.append(by_rows(block, dim))
        ins.append(got)
    if split:
        out_shape = [jax.ShapeDtypeStruct((2 * half, dim), BF16)] * 4
        out_specs = [
            pl.BlockSpec((half, dim), lambda i: (i // 2, 0)),
            pl.BlockSpec((half, dim), lambda i: (jnp.minimum(i, 1), 0)),
            pl.BlockSpec((half, dim), lambda i: (i // 2, 0)),
            pl.BlockSpec((half, dim), lambda i: (jnp.maximum(i - 2, 0), 0)),
        ]
    else:
        out_shape = jax.ShapeDtypeStruct((rows, dim), BF16)
        out_specs = by_rows(block, dim)
    depth = sum(left.shape[1] for left in lefts)
    return pl.pallas_call(
        kernel,
        out_shape=out_shape,
        grid=(steps,),
        in_specs=in_specs,
        out_specs=out_specs,
        compiler_params=params_for(),
        cost_estimate=cost(
            flops=2 * rows * depth * dim,
            bytes_accessed=2 * (rows * depth + depth * dim + 2 * rows * dim),
            transcendentals=0,
        ),
        name="partial_sums",
    )(*ins)


def whole_sums(lefts, rights, place):
    lefts = [columns_of(left) for left in lefts]
    seq = lefts[0].shape[0]
    dim = rights[0].shape[0]
    chunks = place.shape[0]
    block = seq // chunks
    count = len(lefts)

    def kernel(place_ref, *refs):
        total = None
        for left, right in zip(refs[:count], refs[count : 2 * count]):
            term = dot(left[...], right[...], NT)
            total = term if total is None else total + term
        refs[-1][...] = total.astype(BF16)

    depth = sum(left.shape[1] for left in lefts)
    return pl.pallas_call(
        kernel,
        out_shape=jax.ShapeDtypeStruct((seq, dim), BF16),
        grid_spec=pltpu.PrefetchScalarGridSpec(
            num_scalar_prefetch=1,
            grid=(chunks,),
            in_specs=[
                pl.BlockSpec((block, left.shape[1]), lambda i, at, left=left: (at[i], left.index))
                for left in lefts
            ]
            + [resident(right) for right in rights],
            out_specs=pl.BlockSpec((block, dim), lambda i, at: (i, 0)),
        ),
        compiler_params=params_for(),
        cost_estimate=cost(
            flops=2 * seq * depth * dim,
            bytes_accessed=2 * (seq * depth + depth * dim + seq * dim),
            transcendentals=0,
        ),
        name="whole_sums",
    )(place, *[left.array for left in lefts], *[right.array for right in rights])


def halves(array):
    if isinstance(array, (list, tuple)):
        return [(columns_of(half), 0) for half in array]
    return [(columns_of(array), 0), (columns_of(array), 1)]


def weight_grad(lefts, rights, seq):
    seq //= 2
    lefts = [pair for left in lefts for pair in halves(left)]
    rights = [pair for right in rights for pair in halves(right)]
    height = lefts[0][0].shape[1]
    cols = rights[0][0].shape[1]
    tall = min(512 if height <= 1024 else 256, height)
    wide = min(1024, cols)
    count = len(lefts)

    def kernel(*refs):
        total = None
        for left, right in zip(refs[:count], refs[count : 2 * count]):
            term = dot(left[...], right[...], TN)
            total = term if total is None else total + term
        refs[-1][...] = total.astype(BF16)

    def left_spec(part, p):
        first = part.index * (height // tall)
        return pl.BlockSpec((seq, tall), lambda n, m: (p, first + m))

    def right_spec(part, p):
        first = part.index * (cols // wide)
        return pl.BlockSpec((seq, wide), lambda n, m: (p, first + n))

    return pl.pallas_call(
        kernel,
        out_shape=jax.ShapeDtypeStruct((height, cols), BF16),
        grid=(cols // wide, height // tall),
        in_specs=[left_spec(*pair) for pair in lefts] + [right_spec(*pair) for pair in rights],
        out_specs=pl.BlockSpec((tall, wide), lambda n, m: (m, n)),
        compiler_params=params_for(),
        cost_estimate=cost(
            flops=2 * seq * height * cols * count,
            bytes_accessed=2 * count * (seq * height * (cols // wide) + seq * cols),
            transcendentals=0,
        ),
        name="weight_grad",
    )(*[part.array for part, _ in lefts], *[part.array for part, _ in rights])


def head_stack(block, heads):
    lanes = lax.broadcasted_iota(jnp.int32, block.shape, 1) // HEAD_DIM
    zero = jnp.zeros_like(block)
    return jnp.concatenate([jnp.where(lanes == h, block, zero) for h in range(heads)], axis=0)


def block_mask(first_key, first_query, begins, size):
    keys = first_key + lax.broadcasted_iota(jnp.int32, (size, size), 0)
    queries = first_query + lax.broadcasted_iota(jnp.int32, (size, size), 1)
    return (keys <= queries) & (keys >= begins)


def forward_kernel(heads, blocks, size, low_ref, place_ref, begins_ref, qkv_ref, att_ref, lse_ref, vt_ref):
    width = heads * HEAD_DIM

    def spin(b, carry):
        rows = pl.ds(pl.multiple_of(place_ref[b] * size, size), size)
        vt_ref[b] = qkv_ref[rows, 2 * width :].astype(F32).T.astype(BF16)
        return carry

    lax.fori_loop(0, blocks, spin, 0)

    def one_query_block(i, carry):
        rows = pl.ds(pl.multiple_of(place_ref[i] * size, size), size)
        stack = head_stack(qkv_ref[rows, :width], heads)
        begins = begins_ref[i]

        def one_key_block(j, state):
            maxes, totals, sums = state
            keys = pl.ds(pl.multiple_of(place_ref[j] * size, size), size)
            scores = dot(qkv_ref[keys, width : 2 * width], stack, NT)
            allowed = block_mask(j * size, i * size, begins, size)
            new_maxes, new_totals, new_sums = [], [], []
            for h in range(heads):
                part = jnp.where(allowed, scores[:, h * size : (h + 1) * size], NEG)
                peak = jnp.maximum(maxes[h], jnp.max(part, axis=0, keepdims=True))
                fade = jnp.exp(maxes[h] - peak)
                probs = jnp.exp(part - peak)
                new_maxes.append(peak)
                new_totals.append(totals[h] * fade + jnp.sum(probs, axis=0, keepdims=True))
                values_t = vt_ref[j, h * HEAD_DIM : (h + 1) * HEAD_DIM, :]
                new_sums.append(sums[h] * fade + dot(values_t, probs.astype(BF16)))
            return (tuple(new_maxes), tuple(new_totals), tuple(new_sums))

        start = (
            tuple(jnp.full((1, size), NEG, F32) for _ in range(heads)),
            tuple(jnp.zeros((1, size), F32) for _ in range(heads)),
            tuple(jnp.zeros((HEAD_DIM, size), F32) for _ in range(heads)),
        )
        maxes, totals, sums = lax.fori_loop(low_ref[i], i + 1, one_key_block, start)
        outs = jnp.concatenate([sums[h] / totals[h] for h in range(heads)], axis=0)
        att_ref[rows, :] = outs.T.astype(BF16)
        for h in range(heads):
            lse_ref[i, h : h + 1, :] = maxes[h] + jnp.log(totals[h])
        return carry

    lax.fori_loop(0, blocks, one_query_block, 0)


def attend_forward(qkv, low, place, begins, heads):
    seq = qkv.shape[0]
    blocks, _, size = begins.shape
    width = heads * HEAD_DIM
    pairs = seq * seq // 3
    return pl.pallas_call(
        functools.partial(forward_kernel, heads, blocks, size),
        out_shape=(
            jax.ShapeDtypeStruct((seq, width), BF16),
            jax.ShapeDtypeStruct((blocks, heads, size), F32),
        ),
        in_specs=[smem(), smem(), vmem(), vmem()],
        out_specs=(vmem(), vmem()),
        scratch_shapes=[pltpu.VMEM((blocks, width, size), BF16)],
        compiler_params=params_for(),
        cost_estimate=cost(
            flops=16 * pairs * width,
            bytes_accessed=2 * seq * width * 4,
            transcendentals=pairs * heads,
        ),
        name="attend_forward",
    )(low, place, begins, qkv)


def backward_kernel(
    heads,
    blocks,
    size,
    low_ref,
    place_ref,
    begins_ref,
    qkv_ref,
    att_ref,
    grad_ref,
    lse_ref,
    cos_ref,
    sin_ref,
    out_ref,
    kt_ref,
    dk_ref,
    dv_ref,
):
    width = heads * HEAD_DIM
    scale = HEAD_DIM**-0.5

    def spin(b, carry):
        rows = pl.ds(pl.multiple_of(place_ref[b] * size, size), size)
        kt_ref[b] = qkv_ref[rows, width : 2 * width].astype(F32).T.astype(BF16)
        dk_ref[b] = jnp.zeros((size, width), F32)
        dv_ref[b] = jnp.zeros((size, width), F32)
        return carry

    lax.fori_loop(0, blocks, spin, 0)

    def unrotate(values, rows):
        cos = wide_table(cos_ref[rows, :], width)
        sin = wide_table(sin_ref[rows, :], width)
        return values * cos - partner_lanes(values, width) * sin

    def one_query_block(i, carry):
        rows = pl.ds(pl.multiple_of(place_ref[i] * size, size), size)
        q_stack = head_stack(qkv_ref[rows, :width], heads)
        grad = grad_ref[rows, :]
        g_stack = head_stack(grad, heads)
        product = (grad.astype(F32) * att_ref[rows, :].astype(F32)).T
        deltas = [
            jnp.sum(product[h * HEAD_DIM : (h + 1) * HEAD_DIM], axis=0, keepdims=True)
            for h in range(heads)
        ]
        begins = begins_ref[i]

        def one_key_block(j, sums):
            keys = pl.ds(pl.multiple_of(place_ref[j] * size, size), size)
            scores = dot(qkv_ref[keys, width : 2 * width], q_stack, NT)
            grads = dot(qkv_ref[keys, 2 * width :], g_stack, NT)
            allowed = block_mask(j * size, i * size, begins, size)
            all_probs, all_ds, new_sums = [], [], []
            for h in range(heads):
                span = slice(h * size, (h + 1) * size)
                part = jnp.where(allowed, scores[:, span] - lse_ref[i, h : h + 1, :], NEG)
                probs = jnp.exp(part)
                d_scores = (probs * (grads[:, span] - deltas[h])).astype(BF16)
                all_probs.append(probs.astype(BF16))
                all_ds.append(d_scores)
                keys_t = kt_ref[j, h * HEAD_DIM : (h + 1) * HEAD_DIM, :]
                new_sums.append(sums[h] + dot(keys_t, d_scores))
            dv_ref[j] += dot(jnp.concatenate(all_probs, axis=1), g_stack)
            dk_ref[j] += dot(jnp.concatenate(all_ds, axis=1), q_stack)
            return tuple(new_sums)

        start = tuple(jnp.zeros((HEAD_DIM, size), F32) for _ in range(heads))
        sums = lax.fori_loop(low_ref[i], i + 1, one_key_block, start)
        query_grad = jnp.concatenate(sums, axis=0).T * scale
        out_ref[rows, :width] = unrotate(query_grad, rows).astype(BF16)
        return carry

    lax.fori_loop(0, blocks, one_query_block, 0)

    def finish(b, carry):
        rows = pl.ds(pl.multiple_of(place_ref[b] * size, size), size)
        out_ref[rows, width : 2 * width] = unrotate(dk_ref[b], rows).astype(BF16)
        out_ref[rows, 2 * width :] = dv_ref[b].astype(BF16)
        return carry

    lax.fori_loop(0, blocks, finish, 0)


def attend_backward(qkv, att, grad, lse, low, place, begins, cos, sin, heads):
    seq = qkv.shape[0]
    blocks, _, size = begins.shape
    width = heads * HEAD_DIM
    pairs = seq * seq // 3
    return pl.pallas_call(
        functools.partial(backward_kernel, heads, blocks, size),
        out_shape=jax.ShapeDtypeStruct((seq, 3 * width), BF16),
        in_specs=[smem(), smem()] + [vmem()] * 7,
        out_specs=vmem(),
        scratch_shapes=[
            pltpu.VMEM((blocks, width, size), BF16),
            pltpu.VMEM((blocks, size, width), F32),
            pltpu.VMEM((blocks, size, width), F32),
        ],
        compiler_params=params_for(),
        cost_estimate=cost(
            flops=40 * pairs * width,
            bytes_accessed=2 * seq * width * 10,
            transcendentals=pairs * heads,
        ),
        name="attend_backward",
    )(low, place, begins, qkv, att, grad, lse, cos, sin)


def row_facts(lengths, seq):
    wide = lax.axis_size("wide")
    me = lax.axis_index("wide")
    chunk = seq // wide
    docs = lengths.shape[0]
    upto = jnp.arange(docs)[:, None] <= jnp.arange(docs)[None, :]
    ends = jnp.sum(jnp.where(upto, lengths[:, None], 0), axis=0).astype(jnp.int32)

    def starts_of(tokens):
        before = jnp.where(ends[None, :] <= tokens[:, None], ends[None, :], jnp.int32(0))
        return jnp.max(before, axis=1)

    tokens = jnp.arange(seq, dtype=jnp.int32)
    begins = starts_of(tokens).reshape(wide, 1, chunk)
    low = begins[:, 0, 0] // chunk
    index = jnp.arange(wide, dtype=jnp.int32)
    place = place_of(index ^ me, wide)
    owner = me ^ offset_at(index, wide)
    here = (owner[:, None] * chunk + jnp.arange(chunk, dtype=jnp.int32)[None, :]).reshape(seq)
    position = (here - starts_of(here)).astype(F32)
    half_dim = HEAD_DIM // 2
    inverse = ROPE_BASE ** (-(jnp.arange(half_dim, dtype=F32) * 2.0) / HEAD_DIM)
    angles = position[:, None] * inverse[None, :]
    cos = jnp.cos(angles)
    sin = jnp.sin(angles)
    cos = jnp.concatenate([cos, cos, cos, cos], axis=1)
    sin = jnp.concatenate([-sin, sin, -sin, sin], axis=1)
    return low, place, begins, cos, sin


def norm_scale(values):
    return lax.rsqrt(jnp.mean(values * values, axis=-1, keepdims=True) + EPS)


def per_device(
    hidden_in,
    out_grad,
    doc_lengths,
    attn_gain,
    w_query,
    w_key,
    w_value,
    w_out,
    mlp_gain,
    w_gate,
    w_up,
    w_down,
):
    narrow = lax.axis_size("narrow")
    wide = lax.axis_size("wide")
    here = lax.axis_index("narrow")
    rows_here, chunk, dim = hidden_in.shape
    seq = chunk * wide
    width = w_query.shape[1]
    heads = width // HEAD_DIM

    def fetch(weight, axis):
        return lax.all_gather(weight, "narrow", axis=axis, tiled=True)

    gains = jnp.stack([attn_gain, mlp_gain])
    turned = [gains]
    for step in range(1, narrow):
        turned.append(
            lax.ppermute(gains, "narrow", [((i + step) % narrow, i) for i in range(narrow)])
        )
    order = (jnp.arange(narrow) - here) % narrow
    gains = jnp.take(jnp.stack(turned), order, axis=0)
    gains = jnp.swapaxes(gains, 0, 1).reshape(2, dim).astype(F32)
    attn_scale = gains[0]
    mlp_scale = gains[1]

    slots = Slots()
    gate, ends, turn = slots.gate, slots.ends, slots.turn
    hidden = w_gate.shape[1]
    cut = hidden // 2
    spans = [slice(0, cut), slice(cut, hidden)]
    first_own = jnp.concatenate([w_query, w_key, w_value, w_out.T], axis=1)
    first_set = fetch(first_own, 0)
    w_qkv = Columns(first_set, 3 * width, 0)
    full_out = Columns(first_set, width, 3)
    ffn_sets, full_gu, full_down = [], [], []

    def lay_out():
        for span in spans:
            own = [gate(w_gate)[:, span], gate(w_up)[:, span], gate(w_down)[span].T]
            own = ends(jnp.concatenate(own, axis=1))
            ffn_sets.append(fetch(own, 0))
            full_gu.append(Columns(ffn_sets[-1], 2 * cut, 0))
            full_down.append(Columns(ffn_sets[-1], cut, 2))


    rows = range(rows_here)
    last = rows_here - 1
    facts = {}
    residual = [hidden_in[r].astype(F32) for r in rows]
    inv_first = [norm_scale(residual[r]) for r in rows]
    normed = [residual[r] * inv_first[r] for r in rows]
    scaled_in = [(normed[r] * attn_scale).astype(BF16) for r in rows]

    attn_in, gy, mlp_in, branch = {}, {}, {}, {}
    qkv, att, lse, middle, inv_second = ({} for _ in range(5))
    grad_middle, gain_mlp, gain_attn, outputs, in_grads, d_qkv = ({} for _ in range(6))
    hid, d_gu = {}, {}

    def know(r):
        facts[r] = row_facts(gate(doc_lengths[r]), seq)
        ends(facts[r][3])
        ends(facts[r][4])

    def first_of(halves):
        return [gate(halves[0])] + list(halves[1:])

    def project(r):
        _, _, _, cos, sin = facts[r]
        qkv[r] = ends(project_qkv(first_of(attn_in[r].halves), w_qkv, cos, sin))

    def attend(r):
        low, place, begins, _, _ = facts[r]
        att[r], lse[r] = attend_forward(gate(qkv[r]), low, place, begins, heads)
        ends(att[r])

    def spread(lefts, rights):
        return Scatter(slots, lefts, rights)

    def after_attention(r, total):
        middle[r] = gate(hidden_in[r]).astype(F32) + total
        inv_second[r] = norm_scale(middle[r])
        mlp_in[r] = Gather(slots, (middle[r] * inv_second[r] * mlp_scale).astype(BF16))

    def mlp(r):
        hid[r], d_gu[r] = mlp_products(first_of(mlp_in[r].halves), gy[r].halves, ffn_sets)
        ends(hid[r])

    def parts_of(array):
        width = array.shape[1] // len(spans)
        return [Columns(array, width, part) for part in range(len(spans))]

    def after_mlp(r, total):
        total = gate(total).astype(F32)
        normed_mid = gate(middle[r]) * inv_second[r]
        gain_mlp[r] = jnp.sum(total * normed_mid, axis=0)
        scaled = total * mlp_scale
        grad_middle[r] = out_grad[r].astype(F32) + inv_second[r] * (
            scaled - normed_mid * jnp.mean(scaled * normed_mid, axis=-1, keepdims=True)
        )
        branch[r] = Gather(slots, grad_middle[r].astype(BF16))

    def back_attention(r):
        low, place, begins, cos, sin = facts[r]
        grad_att = pull_back_out(first_of(branch[r].halves), full_out)
        d_qkv[r] = ends(
            attend_backward(
                qkv[r], att[r], grad_att, lse[r], low, place, begins, cos, sin, heads
            )
        )

    def after_back(r, total):
        normed_in = gate(hidden_in[r]).astype(F32) * inv_first[r]
        gain_attn[r] = jnp.sum(total * normed_in, axis=0)
        scaled = total * attn_scale
        in_grads[r] = (
            grad_middle[r]
            + inv_first[r]
            * (scaled - normed_in * jnp.mean(scaled * normed_in, axis=-1, keepdims=True))
        ).astype(BF16)

    def grad_factors(lefts, rights):
        lefts = [lefts[r] for r in rows]
        lefts[0] = first_of(lefts[0]) if isinstance(lefts[0], list) else gate(lefts[0])
        return lefts, [rights[r] for r in rows]

    def grad_of(lefts, rights, table, key, wait=True, axis=0):
        grad = ends(weight_grad(*grad_factors(lefts, rights), seq))

        def start():
            table[key] = lax.psum_scatter(
                gate(grad) if wait else grad, "narrow", scatter_dimension=axis, tiled=True
            )

        if wait:
            slots.later(start)
        else:
            start()

    def out_grad_sum():
        grad = ends(weight_grad(*grad_factors(att, halves_of(branch)), seq))

        def start():
            size = grad.shape[1] // narrow

            def block(number):
                return lax.dynamic_slice_in_dim(gate(grad), (number % narrow) * size, size, 1)

            total = block(here).astype(F32)
            for step in range(1, narrow):
                pairs = [(i, (i + step) % narrow) for i in range(narrow)]
                total = total + lax.ppermute(block(here + step), "narrow", pairs).astype(F32)
            grad_attn["out"] = total

        return start

    def both(table):
        return [table[r] for r in rows]

    def halves_of(table):
        return {r: table[r].halves for r in rows}

    sums, down, grad_gu, grad_down, grad_attn = {}, {}, [None, None], [None, None], {}

    def out_sum(r):
        sums[r] = spread([att[r]], [full_out])

    def mlp_sum(r):
        whole = ends(whole_sums(first_of(parts_of(d_gu[r])), full_gu, facts[r][1]))

        def start():
            sums[r] = lax.psum_scatter(gate(whole), "wide", scatter_dimension=0, tiled=True)

        slots.later(start)

    def back_sum(r):
        sums[r] = spread([d_qkv[r]], [w_qkv])

    def down_sum(r):
        down[r] = spread(parts_of(hid[r]), full_down)

    def gu_grad(part):
        grad_of(halves_of(mlp_in), {r: parts_of(d_gu[r])[part] for r in rows}, grad_gu, part)

    def down_grad():
        grad_of(hid, halves_of(gy), grad_down, 0, axis=1)

    one, two = 0, last
    attn_in[one] = Gather(slots, scaled_in[one])
    ends(first_own)
    turn()
    attn_in[one].far()
    know(one)
    lay_out()
    turn()
    attn_in[one].core()
    attn_in[two] = Gather(slots, scaled_in[two])
    know(two)
    ends(first_set)
    turn()
    project(one)
    attn_in[two].far()
    turn()
    attend(one)
    attn_in[two].core()
    gy[one] = Gather(slots, out_grad[one])
    turn()
    out_sum(one)
    sums[one].core()
    project(two)
    gy[one].far()
    turn()
    sums[one].even()
    gy[one].core()
    gy[two] = Gather(slots, out_grad[two])
    turn()
    attend(two)
    sums[one].near()
    ends(ffn_sets[0])
    turn()
    out_sum(two)
    sums[one].last()
    gy[two].far()
    turn()
    after_attention(one, sums[one].total)
    sums[two].core()
    gy[two].core()
    turn()
    sums[two].even()
    mlp_in[one].far()
    turn()
    mlp_in[one].core()
    sums[two].near()
    ends(ffn_sets[1])
    turn()
    mlp(one)
    sums[two].last()
    turn()
    mlp_sum(one)
    after_attention(two, sums[two].total)
    turn()
    down_sum(one)
    down[one].core()
    mlp_in[two].far()
    turn()
    down[one].even()
    mlp_in[two].core()
    turn()
    mlp(two)
    turn()
    mlp_sum(two)
    ends(sums[one])
    turn()
    gu_grad(0)
    after_mlp(one, sums[one])
    turn()
    gu_grad(1)
    branch[one].far()
    turn()
    down_sum(two)
    branch[one].core()
    turn()
    back_attention(one)
    down[one].near()
    down[two].core()
    ends(sums[two])
    turn()
    back_sum(one)
    down[two].even()
    after_mlp(two, sums[two])
    turn()
    down_grad()
    sums[one].core()
    branch[two].far()
    down[one].last()
    turn()
    sums[one].even()
    branch[two].core()
    ends(grad_gu[0])
    turn()
    start_out = out_grad_sum()
    back_attention(two)
    sums[one].near()
    down[two].near()
    turn()
    back_sum(two)
    sums[one].last()
    ends(grad_gu[1])
    turn()
    sums[two].core()
    grad_of(halves_of(attn_in), d_qkv, grad_attn, "qkv", False)
    turn()
    sums[two].even()
    sums[two].near()
    start_out()
    ends(grad_down[0])
    turn()
    sums[two].last()
    down[two].last(False)
    turn()
    for r in rows:
        outputs[r] = (middle[r] + down[r].total).astype(BF16)
        after_back(r, sums[r].total)

    gains = jnp.stack([sum(both(part)[1:], part[one]) for part in (gain_attn, gain_mlp)])
    for axis in ("narrow", "wide"):
        count = lax.axis_size(axis)
        me = lax.axis_index(axis)
        if axis == "wide":
            gains = after(gains, grad_attn["qkv"])
        for bit in reversed(range(bits_of(count))):
            size = gains.shape[1] // 2
            mine = (me >> bit) & 1
            sent = lax.dynamic_slice_in_dim(gains, (1 - mine) * size, size, 1)
            kept = lax.dynamic_slice_in_dim(gains, mine * size, size, 1)
            gains = kept + lax.ppermute(sent, axis, [(i, i ^ (1 << bit)) for i in range(count)])

    grad_gu = [grad.astype(F32) for grad in grad_gu]
    grad_attn = {key: grad.astype(F32) for key, grad in grad_attn.items()}
    grad_gate = [piece[:, :cut] for piece in grad_gu]
    grad_up = [piece[:, cut:] for piece in grad_gu]
    return (
        jnp.stack(both(outputs)),
        jnp.stack(both(in_grads)),
        gains[0],
        grad_attn["qkv"][:, :width],
        grad_attn["qkv"][:, width : 2 * width],
        grad_attn["qkv"][:, 2 * width :],
        grad_attn["out"],
        gains[1],
        jnp.concatenate(grad_gate, axis=1),
        jnp.concatenate(grad_up, axis=1),
        grad_down[0].astype(F32),
    )


def solution(mesh):
    in_specs = (
        P("narrow", "wide", None),
        P("narrow", "wide", None),
        P("narrow", None),
        P("narrow"),
        P("narrow", "wide"),
        P("narrow", "wide"),
        P("narrow", "wide"),
        P("wide", "narrow"),
        P("narrow"),
        P("narrow", "wide"),
        P("narrow", "wide"),
        P("wide", "narrow"),
    )
    out_specs = (
        P("narrow", "wide", None),
        P("narrow", "wide", None),
        P(("narrow", "wide")),
        P("narrow", "wide"),
        P("narrow", "wide"),
        P("narrow", "wide"),
        P("wide", "narrow"),
        P(("narrow", "wide")),
        P("narrow", "wide"),
        P("narrow", "wide"),
        P("wide", "narrow"),
    )
    return jax.shard_map(
        per_device, mesh=mesh, in_specs=in_specs, out_specs=out_specs, check_vma=False
    )
```

```python
import functools

import jax
import jax.numpy as jnp
from jax import lax
from jax.experimental import pallas as pl
from jax.experimental.pallas import tpu as pltpu
from jax.sharding import PartitionSpec as P

HEAD_DIM = 64
EPS = 1e-05
NEG = -1e30
ROPE_BASE = 130000.0
F32 = jnp.float32
BF16 = jnp.bfloat16
NN = (((1,), (0,)), ((), ()))
NT = (((1,), (1,)), ((), ()))
TN = (((0,), (0,)), ((), ()))
VMEM_LIMIT = 60 * 1024 * 1024
COST = 0.02


def dot(left, right, dims=NN):
    return lax.dot_general(left, right, dims, preferred_element_type=F32)


def params_for(**extra):
    return pltpu.CompilerParams(vmem_limit_bytes=VMEM_LIMIT, **extra)


def cost(flops, bytes_accessed, transcendentals):
    return pl.CostEstimate(
        flops=int(flops * COST),
        bytes_accessed=int(bytes_accessed * COST),
        transcendentals=int(transcendentals * COST),
    )


def vmem():
    return pl.BlockSpec(memory_space=pltpu.VMEM)


def smem():
    return pl.BlockSpec(memory_space=pltpu.SMEM)


def bits_of(count):
    return count.bit_length() - 1


def offset_at(place, count):
    top = bits_of(count) - 1
    return ((place << 1) & (count - 1)) | (place >> top)


def place_of(offset, count):
    top = bits_of(count) - 1
    return (offset >> 1) | ((offset & 1) << top)


def swap(block, bit):
    count = lax.axis_size("wide")
    return lax.ppermute(block, "wide", [(i, i ^ (1 << bit)) for i in range(count)])


def after(value, *others):
    return lax.optimization_barrier((value,) + others)[0] if others else value


class Slots:
    def __init__(self):
        self.now = []
        self.then = []
        self.waiting = []

    def later(self, action):
        self.waiting.append(action)

    def gate(self, value):
        if isinstance(value, Columns):
            return Columns(after(value.array, *self.now), value.shape[1], value.index)
        return after(value, *self.now)

    def ends(self, value):
        self.then.append(value)
        return value

    def turn(self):
        self.now = self.then or self.now
        self.then = []
        waiting, self.waiting = self.waiting, []
        for action in waiting:
            action()

    def swap(self, block, bit, axis="wide", hold=True):
        count = lax.axis_size(axis)
        pairs = [(i, i ^ (1 << bit)) for i in range(count)]
        got = lax.ppermute(self.gate(block), axis, pairs)
        return self.ends(got) if hold else got


class Gather:
    def __init__(self, slots, block):
        self.slots = slots
        self.block = block
        chip_bits = bits_of(lax.axis_size("wide")) - 1
        self.plain = not (chip_bits == 2 and block.shape[0] % 32 == 0)
        if not self.plain:
            self.from_x = slots.swap(block, 1)
            self.from_y = slots.swap(block, 2)

    def far(self):
        if not self.plain:
            half = self.block.shape[0] // 2
            self.far_low = self.slots.swap(self.from_y[:half], 1)
            self.far_high = self.slots.swap(self.from_x[half:], 2)

    def core(self):
        if self.plain:
            pieces = [self.block]
            for bit in range(1, bits_of(lax.axis_size("wide"))):
                pieces = pieces + [self.slots.swap(piece, bit) for piece in pieces]
        else:
            pieces = [self.block, self.from_x, self.from_y, self.far_low, self.far_high]
        own = jnp.concatenate(pieces, axis=0)
        self.halves = [own, self.slots.swap(own, 0)]


class Offloaded:
    def __init__(self, slots, block):
        self.slots = slots
        count = lax.axis_size("wide")
        groups = [list(range(core, count, 2)) for core in range(2)]
        self.chips = lax.all_gather(
            slots.gate(block), "wide", axis_index_groups=groups, axis=0, tiled=True
        )

    def core(self):
        chips = lax.axis_size("wide") // 2
        rows = self.chips.shape[0] // chips
        here = lax.axis_index("wide") // 2
        own = jnp.concatenate(
            [
                lax.dynamic_slice_in_dim(self.chips, (here ^ chip) * rows, rows)
                for chip in range(chips)
            ],
            axis=0,
        )
        self.halves = [own, self.slots.swap(own, 0)]


class Scatter:
    def __init__(self, slots, lefts, rights):
        self.slots = slots
        self.factors = (lefts, rights)
        self.sent = self.product(1)

    def product(self, side, got=None):
        lefts, rights = self.factors
        lefts = [self.slots.gate(lefts[0])] + list(lefts[1:])
        made = partial_sums(lefts, rights, side, got)
        self.slots.ends(made[0] if isinstance(made, (list, tuple)) else made)
        return made

    def core(self):
        self.got = self.slots.swap(self.sent, 0)

    def even(self):
        self.kept = self.product(0, self.got)

    def near(self):
        if isinstance(self.kept, (tuple, list)):
            self.got_x = self.slots.swap(self.kept[2], 1)
            self.got_y = self.slots.swap(self.kept[3], 2)
            return
        kept = self.kept
        for bit in reversed(range(bits_of(lax.axis_size("wide")) - 1)):
            rows = kept.shape[0] // 2
            got = self.slots.swap(kept[rows:], bit + 1)
            kept = (kept[:rows].astype(F32) + got.astype(F32)).astype(BF16)
        self.total = kept.astype(F32)

    def last(self, hold=True):
        if not isinstance(self.kept, (tuple, list)):
            return
        keep_low, keep_high = self.kept[:2]
        half = keep_low.shape[0] // 2
        far_low = (keep_low[half:].astype(F32) + self.got_x[half:].astype(F32)).astype(BF16)
        far_high = (keep_high[half:].astype(F32) + self.got_y[half:].astype(F32)).astype(BF16)
        low = self.slots.swap(far_low, 2, hold=hold)
        high = self.slots.swap(far_high, 1, hold=hold)
        low = keep_low[:half].astype(F32) + self.got_x[:half].astype(F32) + low.astype(F32)
        high = keep_high[:half].astype(F32) + self.got_y[:half].astype(F32) + high.astype(F32)
        self.total = jnp.concatenate([low, high], axis=0)


def partner_lanes(values, width):
    lanes = lax.broadcasted_iota(jnp.int32, values.shape, 1)
    first = (lanes % HEAD_DIM) < HEAD_DIM // 2
    half = HEAD_DIM // 2
    return jnp.where(first, pltpu.roll(values, width - half, 1), pltpu.roll(values, half, 1))


def wide_table(table, width):
    copies = width // table.shape[1]
    return jnp.concatenate([table] * copies, axis=1) if copies > 1 else table


def streaming_call(streams, body, ins, in_specs, outs, out_specs, name, flops, moved):
    seq = sum(piece.shape[0] for piece in streams[0])
    rows = min(512, streams[0][0].shape[0])
    steps = seq // rows
    plan = []
    for number, pieces in enumerate(streams):
        first = 0
        for piece in pieces:
            plan.append((number, first, piece.shape[0]))
            first += piece.shape[0]
    count, groups = len(plan), len(streams)

    def kernel(*refs):
        piece_refs, rest = refs[:count], refs[count:]
        middle_refs, buffers, sems = rest[: -groups - 1], rest[-groups - 1 : -1], rest[-1]
        step = pl.program_id(0)

        def copies(block, slot):
            found = []
            for ref, (number, first, size) in zip(piece_refs, plan):
                place = block * rows - first
                if 0 <= place < size:
                    source = ref.at[pl.ds(place, rows)]
                    found.append(
                        pltpu.make_async_copy(
                            source, buffers[number].at[slot], sems.at[number, slot]
                        )
                    )
            return found

        for block in range(steps):

            @pl.when(step == (0 if block == 0 else block - 1))
            def _():
                for copy in copies(block, block % 2):
                    copy.start()

        for block in range(steps):

            @pl.when(step == block)
            def _():
                for copy in copies(block, block % 2):
                    copy.wait()

        slot = lax.rem(step, 2)
        body(*[buffer.at[slot] for buffer in buffers], *middle_refs)

    return pl.pallas_call(
        kernel,
        out_shape=outs,
        grid=(steps,),
        in_specs=[pl.BlockSpec(memory_space=pl.ANY)] * count + in_specs(rows),
        out_specs=out_specs(rows),
        scratch_shapes=[pltpu.VMEM((2, rows, pieces[0].shape[1]), BF16) for pieces in streams]
        + [pltpu.SemaphoreType.DMA((groups, 2))],
        compiler_params=params_for(),
        cost_estimate=cost(
            flops=flops,
            bytes_accessed=moved + sum(2 * seq * pieces[0].shape[1] for pieces in streams),
            transcendentals=0,
        ),
        name=name,
    )(
        *[piece for pieces in streams for piece in pieces],
        *[part.array if isinstance(part, Columns) else part for part in ins],
    )


class Columns:
    def __init__(self, array, width, index):
        self.array = array
        self.index = index
        self.shape = (array.shape[0], width)


def columns_of(array):
    return array if isinstance(array, Columns) else Columns(array, array.shape[1], 0)


def resident(part):
    return pl.BlockSpec(
        part.shape, lambda i, *_: (0, part.index), pipeline_mode=pl.Buffered(1)
    )


def by_rows(rows, cols):
    return pl.BlockSpec((rows, cols), lambda i: (i, 0))


def project_qkv(tokens, weights, cos, sin):
    seq = sum(piece.shape[0] for piece in tokens)
    dim, cols = weights.shape
    width = cols // 3

    def body(x_ref, w_ref, cos_ref, sin_ref, out_ref):
        raw = dot(x_ref[...], w_ref[...])
        cos = wide_table(cos_ref[...], width)
        sin = wide_table(sin_ref[...], width)
        query = raw[:, :width]
        key = raw[:, width : 2 * width]
        query = (query * cos + partner_lanes(query, width) * sin) * (HEAD_DIM**-0.5)
        key = key * cos + partner_lanes(key, width) * sin
        out_ref[:, :width] = query.astype(BF16)
        out_ref[:, width : 2 * width] = key.astype(BF16)
        out_ref[:, 2 * width :] = raw[:, 2 * width :].astype(BF16)

    return streaming_call(
        [tokens],
        body,
        [weights, cos, sin],
        lambda rows: [resident(weights), by_rows(rows, cos.shape[1]), by_rows(rows, sin.shape[1])],
        jax.ShapeDtypeStruct((seq, cols), BF16),
        lambda rows: by_rows(rows, cols),
        "project_qkv",
        2 * seq * dim * cols,
        2 * (dim * cols + seq * cols),
    )


def pull_back_out(tokens, w_out):
    seq = sum(piece.shape[0] for piece in tokens)
    dim, width = w_out.shape

    def body(x_ref, w_ref, out_ref):
        out_ref[...] = dot(x_ref[...], w_ref[...]).astype(BF16)

    return streaming_call(
        [tokens],
        body,
        [w_out],
        lambda rows: [resident(w_out)],
        jax.ShapeDtypeStruct((seq, width), BF16),
        lambda rows: by_rows(rows, width),
        "pull_back_out",
        2 * seq * dim * width,
        2 * (dim * width + seq * width),
    )


def mlp_products(tokens, gy, sets):
    seq = sum(piece.shape[0] for piece in tokens)
    dim = tokens[0].shape[1]
    cut = sets[0].shape[1] // 3
    parts = len(sets)
    rows = min(512, tokens[0].shape[0])
    steps = seq // rows
    streams = [tokens, gy]
    count = sum(len(pieces) for pieces in streams)

    def kernel(*refs):
        piece_refs, set_refs, rest = refs[:count], refs[count : count + parts], refs[count + parts :]
        hid_ref, dgu_ref, x_buffer, gy_buffer, set_buffer, sems, set_sems = rest
        step = pl.program_id(0)

        def copies(number):
            found, at = [], 0
            slot = number % 2
            for stream, (pieces, buffer) in enumerate(zip(streams, (x_buffer, gy_buffer))):
                first = 0
                for piece in pieces:
                    place = (number % steps) * rows - first
                    if 0 <= place < piece.shape[0]:
                        source = piece_refs[at].at[pl.ds(place, rows)]
                        found.append(
                            pltpu.make_async_copy(source, buffer.at[slot], sems.at[stream, slot])
                        )
                    first += piece.shape[0]
                    at += 1
            return found

        loads = [
            pltpu.make_async_copy(set_refs[p], set_buffer.at[p], set_sems.at[p])
            for p in range(parts)
        ]

        @pl.when(step == 0)
        def _():
            for copy in copies(0) + loads:
                copy.start()

        for number in range(parts * steps):

            @pl.when(step == number)
            def _():
                if number + 1 < parts * steps:
                    for copy in copies(number + 1):
                        copy.start()
                for copy in copies(number):
                    copy.wait()
                if number % steps == 0:
                    loads[number // steps].wait()

        slot = lax.rem(step, 2)
        weights = set_buffer.at[step // steps]
        both = dot(x_buffer[slot], weights[:, : 2 * cut])
        d_hid = dot(gy_buffer[slot], weights[:, 2 * cut :])
        gp = both[:, :cut]
        up = both[:, cut:]
        sig = jax.nn.sigmoid(gp)
        silu = gp * sig
        hid_ref[...] = (silu * up).astype(BF16)
        dgu_ref[:, :cut] = (d_hid * up * sig * (1.0 + gp * (1.0 - sig))).astype(BF16)
        dgu_ref[:, cut:] = (d_hid * silu).astype(BF16)

    def out_map(s):
        return (s % steps, s // steps)

    return pl.pallas_call(
        kernel,
        out_shape=[
            jax.ShapeDtypeStruct((seq, parts * cut), BF16),
            jax.ShapeDtypeStruct((seq, 2 * parts * cut), BF16),
        ],
        grid=(parts * steps,),
        in_specs=[pl.BlockSpec(memory_space=pl.ANY)] * (count + parts),
        out_specs=[pl.BlockSpec((rows, cut), out_map), pl.BlockSpec((rows, 2 * cut), out_map)],
        scratch_shapes=[
            pltpu.VMEM((2, rows, dim), BF16),
            pltpu.VMEM((2, rows, dim), BF16),
            pltpu.VMEM((parts, dim, 3 * cut), BF16),
            pltpu.SemaphoreType.DMA((2, 2)),
            pltpu.SemaphoreType.DMA((parts,)),
        ],
        compiler_params=params_for(),
        cost_estimate=cost(
            flops=6 * seq * dim * cut * parts,
            bytes_accessed=2 * parts * (2 * seq * dim + 3 * dim * cut + 3 * seq * cut),
            transcendentals=seq * cut * parts,
        ),
        name="mlp_products",
    )(*[piece for pieces in streams for piece in pieces], *sets)


def partial_sums(lefts, rights, side, got=None):
    lefts = [columns_of(left) for left in lefts]
    seq = lefts[0].shape[0]
    dim = rights[0].shape[0]
    rows = seq // 2
    count = len(lefts)
    wide = lax.axis_size("wide")
    chunk = seq // wide
    split = got is not None and bits_of(wide) == 3 and chunk % 32 == 0
    block = chunk if split else min(512, rows)
    steps = rows // block
    half = block // 2

    def kernel(*refs):
        total = None
        for left, right in zip(refs[:count], refs[count : 2 * count]):
            term = dot(left[...], right[...], NT)
            total = term if total is None else total + term
        if got is None:
            refs[-1][...] = total.astype(BF16)
            return
        total = total + refs[2 * count][...].astype(F32)
        if not split:
            refs[-1][...] = total.astype(BF16)
            return
        keep_low, keep_high, send_x, send_y = refs[-4:]
        step = pl.program_id(0)
        low = total[:half].astype(BF16)
        high = total[half:].astype(BF16)

        @pl.when(step % 2 == 0)
        def _():
            keep_low[...] = low

        @pl.when(step % 2 == 1)
        def _():
            send_x[...] = low

        @pl.when(step < 2)
        def _():
            keep_high[...] = high

        @pl.when(step >= 2)
        def _():
            send_y[...] = high

    in_specs = [
        pl.BlockSpec((block, left.shape[1]), lambda i, left=left: (side * steps + i, left.index))
        for left in lefts
    ] + [resident(right) for right in rights]
    ins = [left.array for left in lefts] + [right.array for right in rights]
    if got is not None:
        in_specs.append(by_rows(block, dim))
        ins.append(got)
    if split:
        out_shape = [jax.ShapeDtypeStruct((2 * half, dim), BF16)] * 4
        out_specs = [
            pl.BlockSpec((half, dim), lambda i: (i // 2, 0)),
            pl.BlockSpec((half, dim), lambda i: (jnp.minimum(i, 1), 0)),
            pl.BlockSpec((half, dim), lambda i: (i // 2, 0)),
            pl.BlockSpec((half, dim), lambda i: (jnp.maximum(i - 2, 0), 0)),
        ]
    else:
        out_shape = jax.ShapeDtypeStruct((rows, dim), BF16)
        out_specs = by_rows(block, dim)
    depth = sum(left.shape[1] for left in lefts)
    return pl.pallas_call(
        kernel,
        out_shape=out_shape,
        grid=(steps,),
        in_specs=in_specs,
        out_specs=out_specs,
        compiler_params=params_for(),
        cost_estimate=cost(
            flops=2 * rows * depth * dim,
            bytes_accessed=2 * (rows * depth + depth * dim + 2 * rows * dim),
            transcendentals=0,
        ),
        name="partial_sums",
    )(*ins)


def whole_sums(lefts, rights, place):
    lefts = [columns_of(left) for left in lefts]
    seq = lefts[0].shape[0]
    dim = rights[0].shape[0]
    chunks = place.shape[0]
    block = seq // chunks
    count = len(lefts)

    def kernel(place_ref, *refs):
        total = None
        for left, right in zip(refs[:count], refs[count : 2 * count]):
            term = dot(left[...], right[...], NT)
            total = term if total is None else total + term
        refs[-1][...] = total.astype(BF16)

    depth = sum(left.shape[1] for left in lefts)
    return pl.pallas_call(
        kernel,
        out_shape=jax.ShapeDtypeStruct((seq, dim), BF16),
        grid_spec=pltpu.PrefetchScalarGridSpec(
            num_scalar_prefetch=1,
            grid=(chunks,),
            in_specs=[
                pl.BlockSpec((block, left.shape[1]), lambda i, at, left=left: (at[i], left.index))
                for left in lefts
            ]
            + [resident(right) for right in rights],
            out_specs=pl.BlockSpec((block, dim), lambda i, at: (i, 0)),
        ),
        compiler_params=params_for(),
        cost_estimate=cost(
            flops=2 * seq * depth * dim,
            bytes_accessed=2 * (seq * depth + depth * dim + seq * dim),
            transcendentals=0,
        ),
        name="whole_sums",
    )(place, *[left.array for left in lefts], *[right.array for right in rights])


def halves(array):
    if isinstance(array, (list, tuple)):
        return [(columns_of(half), 0) for half in array]
    return [(columns_of(array), 0), (columns_of(array), 1)]


def weight_grad(lefts, rights, seq):
    seq //= 2
    lefts = [pair for left in lefts for pair in halves(left)]
    rights = [pair for right in rights for pair in halves(right)]
    height = lefts[0][0].shape[1]
    cols = rights[0][0].shape[1]
    tall = min(512 if height <= 1024 else 256, height)
    wide = min(1024, cols)
    count = len(lefts)

    def kernel(*refs):
        total = None
        for left, right in zip(refs[:count], refs[count : 2 * count]):
            term = dot(left[...], right[...], TN)
            total = term if total is None else total + term
        refs[-1][...] = total.astype(BF16)

    def left_spec(part, p):
        first = part.index * (height // tall)
        return pl.BlockSpec((seq, tall), lambda n, m: (p, first + m))

    def right_spec(part, p):
        first = part.index * (cols // wide)
        return pl.BlockSpec((seq, wide), lambda n, m: (p, first + n))

    return pl.pallas_call(
        kernel,
        out_shape=jax.ShapeDtypeStruct((height, cols), BF16),
        grid=(cols // wide, height // tall),
        in_specs=[left_spec(*pair) for pair in lefts] + [right_spec(*pair) for pair in rights],
        out_specs=pl.BlockSpec((tall, wide), lambda n, m: (m, n)),
        compiler_params=params_for(),
        cost_estimate=cost(
            flops=2 * seq * height * cols * count,
            bytes_accessed=2 * count * (seq * height * (cols // wide) + seq * cols),
            transcendentals=0,
        ),
        name="weight_grad",
    )(*[part.array for part, _ in lefts], *[part.array for part, _ in rights])


def head_stack(block, heads):
    lanes = lax.broadcasted_iota(jnp.int32, block.shape, 1) // HEAD_DIM
    zero = jnp.zeros_like(block)
    return jnp.concatenate([jnp.where(lanes == h, block, zero) for h in range(heads)], axis=0)


def block_mask(first_key, first_query, begins, size):
    keys = first_key + lax.broadcasted_iota(jnp.int32, (size, size), 0)
    queries = first_query + lax.broadcasted_iota(jnp.int32, (size, size), 1)
    return (keys <= queries) & (keys >= begins)


def forward_kernel(heads, blocks, size, low_ref, place_ref, begins_ref, qkv_ref, att_ref, lse_ref, vt_ref):
    width = heads * HEAD_DIM

    def spin(b, carry):
        rows = pl.ds(pl.multiple_of(place_ref[b] * size, size), size)
        vt_ref[b] = qkv_ref[rows, 2 * width :].astype(F32).T.astype(BF16)
        return carry

    lax.fori_loop(0, blocks, spin, 0)

    def one_query_block(i, carry):
        rows = pl.ds(pl.multiple_of(place_ref[i] * size, size), size)
        stack = head_stack(qkv_ref[rows, :width], heads)
        begins = begins_ref[i]

        def one_key_block(j, state):
            maxes, totals, sums = state
            keys = pl.ds(pl.multiple_of(place_ref[j] * size, size), size)
            scores = dot(qkv_ref[keys, width : 2 * width], stack, NT)
            allowed = block_mask(j * size, i * size, begins, size)
            new_maxes, new_totals, new_sums = [], [], []
            for h in range(heads):
                part = jnp.where(allowed, scores[:, h * size : (h + 1) * size], NEG)
                peak = jnp.maximum(maxes[h], jnp.max(part, axis=0, keepdims=True))
                fade = jnp.exp(maxes[h] - peak)
                probs = jnp.exp(part - peak)
                new_maxes.append(peak)
                new_totals.append(totals[h] * fade + jnp.sum(probs, axis=0, keepdims=True))
                values_t = vt_ref[j, h * HEAD_DIM : (h + 1) * HEAD_DIM, :]
                new_sums.append(sums[h] * fade + dot(values_t, probs.astype(BF16)))
            return (tuple(new_maxes), tuple(new_totals), tuple(new_sums))

        start = (
            tuple(jnp.full((1, size), NEG, F32) for _ in range(heads)),
            tuple(jnp.zeros((1, size), F32) for _ in range(heads)),
            tuple(jnp.zeros((HEAD_DIM, size), F32) for _ in range(heads)),
        )
        maxes, totals, sums = lax.fori_loop(low_ref[i], i + 1, one_key_block, start)
        outs = jnp.concatenate([sums[h] / totals[h] for h in range(heads)], axis=0)
        att_ref[rows, :] = outs.T.astype(BF16)
        for h in range(heads):
            lse_ref[i, h : h + 1, :] = maxes[h] + jnp.log(totals[h])
        return carry

    lax.fori_loop(0, blocks, one_query_block, 0)


def attend_forward(qkv, low, place, begins, heads):
    seq = qkv.shape[0]
    blocks, _, size = begins.shape
    width = heads * HEAD_DIM
    pairs = seq * seq // 3
    return pl.pallas_call(
        functools.partial(forward_kernel, heads, blocks, size),
        out_shape=(
            jax.ShapeDtypeStruct((seq, width), BF16),
            jax.ShapeDtypeStruct((blocks, heads, size), F32),
        ),
        in_specs=[smem(), smem(), vmem(), vmem()],
        out_specs=(vmem(), vmem()),
        scratch_shapes=[pltpu.VMEM((blocks, width, size), BF16)],
        compiler_params=params_for(),
        cost_estimate=cost(
            flops=16 * pairs * width,
            bytes_accessed=2 * seq * width * 4,
            transcendentals=pairs * heads,
        ),
        name="attend_forward",
    )(low, place, begins, qkv)


def backward_kernel(
    heads,
    blocks,
    size,
    low_ref,
    place_ref,
    begins_ref,
    qkv_ref,
    att_ref,
    grad_ref,
    lse_ref,
    cos_ref,
    sin_ref,
    out_ref,
    kt_ref,
    dk_ref,
    dv_ref,
):
    width = heads * HEAD_DIM
    scale = HEAD_DIM**-0.5

    def spin(b, carry):
        rows = pl.ds(pl.multiple_of(place_ref[b] * size, size), size)
        kt_ref[b] = qkv_ref[rows, width : 2 * width].astype(F32).T.astype(BF16)
        dk_ref[b] = jnp.zeros((size, width), F32)
        dv_ref[b] = jnp.zeros((size, width), F32)
        return carry

    lax.fori_loop(0, blocks, spin, 0)

    def unrotate(values, rows):
        cos = wide_table(cos_ref[rows, :], width)
        sin = wide_table(sin_ref[rows, :], width)
        return values * cos - partner_lanes(values, width) * sin

    def one_query_block(i, carry):
        rows = pl.ds(pl.multiple_of(place_ref[i] * size, size), size)
        q_stack = head_stack(qkv_ref[rows, :width], heads)
        grad = grad_ref[rows, :]
        g_stack = head_stack(grad, heads)
        product = (grad.astype(F32) * att_ref[rows, :].astype(F32)).T
        deltas = [
            jnp.sum(product[h * HEAD_DIM : (h + 1) * HEAD_DIM], axis=0, keepdims=True)
            for h in range(heads)
        ]
        begins = begins_ref[i]

        def one_key_block(j, sums):
            keys = pl.ds(pl.multiple_of(place_ref[j] * size, size), size)
            scores = dot(qkv_ref[keys, width : 2 * width], q_stack, NT)
            grads = dot(qkv_ref[keys, 2 * width :], g_stack, NT)
            allowed = block_mask(j * size, i * size, begins, size)
            all_probs, all_ds, new_sums = [], [], []
            for h in range(heads):
                span = slice(h * size, (h + 1) * size)
                part = jnp.where(allowed, scores[:, span] - lse_ref[i, h : h + 1, :], NEG)
                probs = jnp.exp(part)
                d_scores = (probs * (grads[:, span] - deltas[h])).astype(BF16)
                all_probs.append(probs.astype(BF16))
                all_ds.append(d_scores)
                keys_t = kt_ref[j, h * HEAD_DIM : (h + 1) * HEAD_DIM, :]
                new_sums.append(sums[h] + dot(keys_t, d_scores))
            dv_ref[j] += dot(jnp.concatenate(all_probs, axis=1), g_stack)
            dk_ref[j] += dot(jnp.concatenate(all_ds, axis=1), q_stack)
            return tuple(new_sums)

        start = tuple(jnp.zeros((HEAD_DIM, size), F32) for _ in range(heads))
        sums = lax.fori_loop(low_ref[i], i + 1, one_key_block, start)
        query_grad = jnp.concatenate(sums, axis=0).T * scale
        out_ref[rows, :width] = unrotate(query_grad, rows).astype(BF16)
        return carry

    lax.fori_loop(0, blocks, one_query_block, 0)

    def finish(b, carry):
        rows = pl.ds(pl.multiple_of(place_ref[b] * size, size), size)
        out_ref[rows, width : 2 * width] = unrotate(dk_ref[b], rows).astype(BF16)
        out_ref[rows, 2 * width :] = dv_ref[b].astype(BF16)
        return carry

    lax.fori_loop(0, blocks, finish, 0)


def attend_backward(qkv, att, grad, lse, low, place, begins, cos, sin, heads):
    seq = qkv.shape[0]
    blocks, _, size = begins.shape
    width = heads * HEAD_DIM
    pairs = seq * seq // 3
    return pl.pallas_call(
        functools.partial(backward_kernel, heads, blocks, size),
        out_shape=jax.ShapeDtypeStruct((seq, 3 * width), BF16),
        in_specs=[smem(), smem()] + [vmem()] * 7,
        out_specs=vmem(),
        scratch_shapes=[
            pltpu.VMEM((blocks, width, size), BF16),
            pltpu.VMEM((blocks, size, width), F32),
            pltpu.VMEM((blocks, size, width), F32),
        ],
        compiler_params=params_for(),
        cost_estimate=cost(
            flops=40 * pairs * width,
            bytes_accessed=2 * seq * width * 10,
            transcendentals=pairs * heads,
        ),
        name="attend_backward",
    )(low, place, begins, qkv, att, grad, lse, cos, sin)


def row_facts(lengths, seq):
    wide = lax.axis_size("wide")
    me = lax.axis_index("wide")
    chunk = seq // wide
    docs = lengths.shape[0]
    upto = jnp.arange(docs)[:, None] <= jnp.arange(docs)[None, :]
    ends = jnp.sum(jnp.where(upto, lengths[:, None], 0), axis=0).astype(jnp.int32)

    def starts_of(tokens):
        before = jnp.where(ends[None, :] <= tokens[:, None], ends[None, :], jnp.int32(0))
        return jnp.max(before, axis=1)

    tokens = jnp.arange(seq, dtype=jnp.int32)
    begins = starts_of(tokens).reshape(wide, 1, chunk)
    low = begins[:, 0, 0] // chunk
    index = jnp.arange(wide, dtype=jnp.int32)
    place = place_of(index ^ me, wide)
    owner = me ^ offset_at(index, wide)
    here = (owner[:, None] * chunk + jnp.arange(chunk, dtype=jnp.int32)[None, :]).reshape(seq)
    position = (here - starts_of(here)).astype(F32)
    half_dim = HEAD_DIM // 2
    inverse = ROPE_BASE ** (-(jnp.arange(half_dim, dtype=F32) * 2.0) / HEAD_DIM)
    angles = position[:, None] * inverse[None, :]
    cos = jnp.cos(angles)
    sin = jnp.sin(angles)
    cos = jnp.concatenate([cos, cos, cos, cos], axis=1)
    sin = jnp.concatenate([-sin, sin, -sin, sin], axis=1)
    return low, place, begins, cos, sin


def norm_scale(values):
    return lax.rsqrt(jnp.mean(values * values, axis=-1, keepdims=True) + EPS)


def per_device(
    hidden_in,
    out_grad,
    doc_lengths,
    attn_gain,
    w_query,
    w_key,
    w_value,
    w_out,
    mlp_gain,
    w_gate,
    w_up,
    w_down,
):
    narrow = lax.axis_size("narrow")
    wide = lax.axis_size("wide")
    here = lax.axis_index("narrow")
    rows_here, chunk, dim = hidden_in.shape
    seq = chunk * wide
    width = w_query.shape[1]
    heads = width // HEAD_DIM

    def fetch(weight, axis):
        return lax.all_gather(weight, "narrow", axis=axis, tiled=True)

    gains = jnp.stack([attn_gain, mlp_gain])
    turned = [gains]
    for step in range(1, narrow):
        turned.append(
            lax.ppermute(gains, "narrow", [((i + step) % narrow, i) for i in range(narrow)])
        )
    order = (jnp.arange(narrow) - here) % narrow
    gains = jnp.take(jnp.stack(turned), order, axis=0)
    gains = jnp.swapaxes(gains, 0, 1).reshape(2, dim).astype(F32)
    attn_scale = gains[0]
    mlp_scale = gains[1]

    slots = Slots()
    gate, ends, turn = slots.gate, slots.ends, slots.turn
    hidden = w_gate.shape[1]
    cut = hidden // 2
    spans = [slice(0, cut), slice(cut, hidden)]
    first_own = jnp.concatenate([w_query, w_key, w_value, w_out.T], axis=1)
    first_set = fetch(first_own, 0)
    w_qkv = Columns(first_set, 3 * width, 0)
    full_out = Columns(first_set, width, 3)
    ffn_sets, full_gu, full_down = [], [], []

    def lay_out():
        for span in spans:
            own = [gate(w_gate)[:, span], gate(w_up)[:, span], gate(w_down)[span].T]
            own = ends(jnp.concatenate(own, axis=1))
            ffn_sets.append(fetch(own, 0))
            full_gu.append(Columns(ffn_sets[-1], 2 * cut, 0))
            full_down.append(Columns(ffn_sets[-1], cut, 2))


    rows = range(rows_here)
    last = rows_here - 1
    facts = {}
    residual = [hidden_in[r].astype(F32) for r in rows]
    inv_first = [norm_scale(residual[r]) for r in rows]
    normed = [residual[r] * inv_first[r] for r in rows]
    scaled_in = [(normed[r] * attn_scale).astype(BF16) for r in rows]

    attn_in, gy, mlp_in, branch = {}, {}, {}, {}
    qkv, att, lse, middle, inv_second = ({} for _ in range(5))
    grad_middle, gain_mlp, gain_attn, outputs, in_grads, d_qkv = ({} for _ in range(6))
    hid, d_gu = {}, {}

    def know(r):
        facts[r] = row_facts(gate(doc_lengths[r]), seq)
        ends(facts[r][3])
        ends(facts[r][4])

    def first_of(halves):
        return [gate(halves[0])] + list(halves[1:])

    def project(r):
        _, _, _, cos, sin = facts[r]
        qkv[r] = ends(project_qkv(first_of(attn_in[r].halves), w_qkv, cos, sin))

    def attend(r):
        low, place, begins, _, _ = facts[r]
        att[r], lse[r] = attend_forward(gate(qkv[r]), low, place, begins, heads)
        ends(att[r])

    def spread(lefts, rights):
        return Scatter(slots, lefts, rights)

    def after_attention(r, total):
        middle[r] = gate(hidden_in[r]).astype(F32) + total
        inv_second[r] = norm_scale(middle[r])
        mlp_in[r] = Gather(slots, (middle[r] * inv_second[r] * mlp_scale).astype(BF16))

    def mlp(r):
        hid[r], d_gu[r] = mlp_products(first_of(mlp_in[r].halves), gy[r].halves, ffn_sets)
        ends(hid[r])

    def parts_of(array):
        width = array.shape[1] // len(spans)
        return [Columns(array, width, part) for part in range(len(spans))]

    def after_mlp(r, total):
        total = gate(total).astype(F32)
        normed_mid = gate(middle[r]) * inv_second[r]
        gain_mlp[r] = jnp.sum(total * normed_mid, axis=0)
        scaled = total * mlp_scale
        grad_middle[r] = out_grad[r].astype(F32) + inv_second[r] * (
            scaled - normed_mid * jnp.mean(scaled * normed_mid, axis=-1, keepdims=True)
        )
        branch[r] = Gather(slots, grad_middle[r].astype(BF16))

    def back_attention(r):
        low, place, begins, cos, sin = facts[r]
        grad_att = pull_back_out(first_of(branch[r].halves), full_out)
        d_qkv[r] = ends(
            attend_backward(
                qkv[r], att[r], grad_att, lse[r], low, place, begins, cos, sin, heads
            )
        )

    def after_back(r, total):
        normed_in = gate(hidden_in[r]).astype(F32) * inv_first[r]
        gain_attn[r] = jnp.sum(total * normed_in, axis=0)
        scaled = total * attn_scale
        in_grads[r] = (
            grad_middle[r]
            + inv_first[r]
            * (scaled - normed_in * jnp.mean(scaled * normed_in, axis=-1, keepdims=True))
        ).astype(BF16)

    def grad_factors(lefts, rights):
        lefts = [lefts[r] for r in rows]
        lefts[0] = first_of(lefts[0]) if isinstance(lefts[0], list) else gate(lefts[0])
        return lefts, [rights[r] for r in rows]

    def grad_of(lefts, rights, table, key, wait=True, axis=0):
        grad = ends(weight_grad(*grad_factors(lefts, rights), seq))

        def start():
            table[key] = lax.psum_scatter(
                gate(grad) if wait else grad, "narrow", scatter_dimension=axis, tiled=True
            )

        if wait:
            slots.later(start)
        else:
            start()

    def out_grad_sum():
        grad = ends(weight_grad(*grad_factors(att, halves_of(branch)), seq))

        def start():
            size = grad.shape[1] // narrow

            def block(number):
                return lax.dynamic_slice_in_dim(gate(grad), (number % narrow) * size, size, 1)

            pieces = [block(here)]
            for step in range(1, narrow):
                pairs = [(i, (i + step) % narrow) for i in range(narrow)]
                pieces.append(lax.ppermute(block(here + step), "narrow", pairs))
            grad_attn["out"] = pieces

        return start

    def both(table):
        return [table[r] for r in rows]

    def halves_of(table):
        return {r: table[r].halves for r in rows}

    sums, down, grad_gu, grad_down, grad_attn = {}, {}, [None, None], [None, None], {}

    def out_sum(r):
        sums[r] = spread([att[r]], [full_out])

    def mlp_sum(r):
        whole = ends(whole_sums(first_of(parts_of(d_gu[r])), full_gu, facts[r][1]))

        def start():
            sums[r] = lax.psum_scatter(gate(whole), "wide", scatter_dimension=0, tiled=True)

        slots.later(start)

    def back_sum(r):
        sums[r] = spread([d_qkv[r]], [w_qkv])

    def down_sum(r):
        down[r] = spread(parts_of(hid[r]), full_down)

    def gu_grad(part):
        grad_of(halves_of(mlp_in), {r: parts_of(d_gu[r])[part] for r in rows}, grad_gu, part)

    def down_grad():
        grad_of(hid, halves_of(gy), grad_down, 0, axis=1)

    one, two = 0, last
    attn_in[one] = Gather(slots, scaled_in[one])
    ends(first_own)
    turn()
    attn_in[one].far()
    know(one)
    lay_out()
    turn()
    attn_in[one].core()
    attn_in[two] = Gather(slots, scaled_in[two])
    know(two)
    ends(first_set)
    turn()
    project(one)
    attn_in[two].far()
    turn()
    attend(one)
    attn_in[two].core()
    gy[one] = Gather(slots, out_grad[one])
    turn()
    out_sum(one)
    sums[one].core()
    project(two)
    gy[one].far()
    turn()
    sums[one].even()
    gy[one].core()
    gy[two] = Gather(slots, out_grad[two])
    turn()
    attend(two)
    sums[one].near()
    ends(ffn_sets[0])
    turn()
    out_sum(two)
    sums[one].last()
    gy[two].far()
    turn()
    after_attention(one, sums[one].total)
    sums[two].core()
    gy[two].core()
    turn()
    sums[two].even()
    mlp_in[one].far()
    turn()
    mlp_in[one].core()
    sums[two].near()
    ends(ffn_sets[1])
    turn()
    mlp(one)
    sums[two].last()
    turn()
    mlp_sum(one)
    after_attention(two, sums[two].total)
    turn()
    down_sum(one)
    down[one].core()
    mlp_in[two].far()
    turn()
    down[one].even()
    mlp_in[two].core()
    turn()
    mlp(two)
    turn()
    mlp_sum(two)
    ends(sums[one])
    turn()
    gu_grad(0)
    after_mlp(one, sums[one])
    turn()
    gu_grad(1)
    branch[one].far()
    turn()
    down_sum(two)
    branch[one].core()
    turn()
    back_attention(one)
    down[one].near()
    down[two].core()
    ends(sums[two])
    turn()
    back_sum(one)
    down[two].even()
    after_mlp(two, sums[two])
    turn()
    down_grad()
    sums[one].core()
    branch[two].far()
    down[one].last()
    turn()
    sums[one].even()
    branch[two].core()
    ends(grad_gu[0])
    turn()
    start_out = out_grad_sum()
    back_attention(two)
    sums[one].near()
    down[two].near()
    turn()
    back_sum(two)
    sums[one].last()
    ends(grad_gu[1])
    turn()
    sums[two].core()
    grad_of(halves_of(attn_in), d_qkv, grad_attn, "qkv", False)
    turn()
    sums[two].even()
    sums[two].near()
    start_out()
    ends(grad_down[0])
    turn()
    sums[two].last()
    down[two].last(False)
    turn()
    pieces = [gate(piece).astype(F32) for piece in grad_attn["out"]]
    grad_attn["out"] = sum(pieces[1:], pieces[0])
    for r in rows:
        outputs[r] = (middle[r] + down[r].total).astype(BF16)
        after_back(r, sums[r].total)

    gains = jnp.stack([sum(both(part)[1:], part[one]) for part in (gain_attn, gain_mlp)])
    for axis in ("narrow", "wide"):
        count = lax.axis_size(axis)
        me = lax.axis_index(axis)
        if axis == "wide":
            gains = after(gains, grad_attn["qkv"])
        for bit in reversed(range(bits_of(count))):
            size = gains.shape[1] // 2
            mine = (me >> bit) & 1
            sent = lax.dynamic_slice_in_dim(gains, (1 - mine) * size, size, 1)
            kept = lax.dynamic_slice_in_dim(gains, mine * size, size, 1)
            gains = kept + lax.ppermute(sent, axis, [(i, i ^ (1 << bit)) for i in range(count)])

    grad_gu = [grad.astype(F32) for grad in grad_gu]
    grad_attn = {key: grad.astype(F32) for key, grad in grad_attn.items()}
    grad_gate = [piece[:, :cut] for piece in grad_gu]
    grad_up = [piece[:, cut:] for piece in grad_gu]
    return (
        jnp.stack(both(outputs)),
        jnp.stack(both(in_grads)),
        gains[0],
        grad_attn["qkv"][:, :width],
        grad_attn["qkv"][:, width : 2 * width],
        grad_attn["qkv"][:, 2 * width :],
        grad_attn["out"],
        gains[1],
        jnp.concatenate(grad_gate, axis=1),
        jnp.concatenate(grad_up, axis=1),
        grad_down[0].astype(F32),
    )


def solution(mesh):
    in_specs = (
        P("narrow", "wide", None),
        P("narrow", "wide", None),
        P("narrow", None),
        P("narrow"),
        P("narrow", "wide"),
        P("narrow", "wide"),
        P("narrow", "wide"),
        P("wide", "narrow"),
        P("narrow"),
        P("narrow", "wide"),
        P("narrow", "wide"),
        P("wide", "narrow"),
    )
    out_specs = (
        P("narrow", "wide", None),
        P("narrow", "wide", None),
        P(("narrow", "wide")),
        P("narrow", "wide"),
        P("narrow", "wide"),
        P("narrow", "wide"),
        P("wide", "narrow"),
        P(("narrow", "wide")),
        P("narrow", "wide"),
        P("narrow", "wide"),
        P("wide", "narrow"),
    )
    return jax.shard_map(
        per_device, mesh=mesh, in_specs=in_specs, out_specs=out_specs, check_vma=False
    )
```
